256 devices in a mesh: ta: 64 (over y, z_hi, x, core), ga: 4 (over z_lo).
Axes of the slice: x: 4, y: 4, z: 8 (z_hi: 2, z_lo: 4; z = z_hi * 4 + z_lo), core: 2. Of those that a mesh axis runs over, the one named last changes fastest.
Arguments:
- snapshots: bfloat16 [1024, 4, 131072], P('ta', 'ga'), may hold values from -12 to 12
- block_starts: int32 [7], replicated, may hold values from 0 to 768
- kept_freqs: int32 [32], replicated, may hold values from 0 to 128
Outputs:
- spectra: bfloat16 [4, 7, 2, 32, 131072], P('ga', None, None, None, 'ta')
- power_step: float32 [4, 7, 2, 32, 131072], P('ga', None, None, None, 'ta')
The draws below stay inside these ranges and needn't reach their ends.
All inputs are finite; a program needn't handle non-finite values.
Results may differ from the reference program's by a relative error of at most 0.0047.
Values may be sent and summed in bfloat16 or wider, within the bound.
No kernel may reach another device: no remote copies, remote signals or barrier semaphores. Data moves between devices by JAX's collectives and lax.ppermute only.
A program may use at most 192 MiB of HBM per device.

```python
import math
import jax
import jax.numpy as jnp
from jax import lax

NT = 1024
NFFT = 256
NB = 7
NF = 32
GROUPS = 4
GROUP_PTS = 131072


def draw_snapshots(key, part):
    key_noise = jax.random.fold_in(key, 11)
    key_rough = jax.random.fold_in(key, 12)
    total_pts = GROUPS * GROUP_PTS
    position = jnp.arange(total_pts, dtype=jnp.float32) / (total_pts - 1)
    roughness = jax.random.uniform(key_rough, (total_pts,), jnp.float32, 0.7, 1.4)
    amplitude = roughness * jnp.exp(position * (0.5 * math.log(3.0)))
    values = amplitude[None, :] * jax.random.normal(key_noise, (NT, total_pts), jnp.float32)
    values = jnp.clip(values, -12.0, 12.0)
    return values.reshape(NT, GROUPS, GROUP_PTS).astype(jnp.bfloat16)


def with_ends(entries, rng, low, largest):
    place = [jax.random.randint(jax.random.fold_in(rng, axis), (), 0, length) for axis, length in enumerate(entries.shape)]
    main_axis = entries.shape.index(max(entries.shape))
    neighbour = place[:main_axis] + [(place[main_axis] + 1) % entries.shape[main_axis]] + place[main_axis + 1:]
    return entries.at[tuple(place)].set(low).at[tuple(neighbour)].set(largest)


def setup_inputs(seed: int = 0) -> dict:
    streams_of = jax.random.split(jax.random.key(seed), 4)
    snapshots = draw_snapshots(jax.random.fold_in(streams_of[3], 71), 0)
    block_starts = with_ends(jax.random.randint(streams_of[1], (NB,), 0, NT - NFFT + 1), jax.random.fold_in(streams_of[1], 1), 0, NT - NFFT).astype(jnp.int32)
    kept_freqs = with_ends(jax.random.randint(streams_of[2], (NF,), 0, NFFT // 2 + 1), jax.random.fold_in(streams_of[2], 1), 0, (NFFT // 2 + 1) - 1).astype(jnp.int32)
    return {"snapshots": snapshots, "block_starts": block_starts, "kept_freqs": kept_freqs}


def kernel_table(kept_freqs, sample_index):
    phase_index = kept_freqs[:, None] * sample_index[None, :] % NFFT
    angle_val = 2.0 * math.pi / NFFT * phase_index.astype(jnp.float32)
    window = 0.5 - 0.5 * jnp.cos(2.0 * math.pi / NFFT * sample_index.astype(jnp.float32))
    norm_scale = 2.0 / math.sqrt(NFFT)
    real_rows = window[None, :] * jnp.cos(angle_val) * norm_scale
    imag_rows = -window[None, :] * jnp.sin(angle_val) * norm_scale
    return jnp.concatenate([real_rows, imag_rows], axis=0)

def reference(snapshots, block_starts, kept_freqs):
    total_pts = GROUPS * GROUP_PTS
    series = snapshots.reshape(NT, total_pts)
    kernel_rows = kernel_table(kept_freqs, jnp.arange(NFFT, dtype=jnp.int32)).astype(jnp.bfloat16)
    blocks = []
    for block_index in range(NB):
        segment = lax.dynamic_slice_in_dim(series, block_starts[block_index].astype(jnp.int32), NFFT, 0)
        blocks.append(jnp.dot(kernel_rows, segment, preferred_element_type=jnp.float32).astype(jnp.bfloat16))
    spectra = jnp.stack(blocks)
    values = spectra.astype(jnp.float32).reshape(NB, 2, NF, total_pts)
    real_part = values[:, 0]
    imag_part = values[:, 1]
    highest = lax.Precision.HIGHEST
    denominator = float(NB * total_pts)
    gram_re = (jnp.einsum('bfp,cfp->fbc', real_part, real_part, precision=highest) + jnp.einsum('bfp,cfp->fbc', imag_part, imag_part, precision=highest)) / denominator
    gram_im = (jnp.einsum('bfp,cfp->fbc', real_part, imag_part, precision=highest) - jnp.einsum('bfp,cfp->fbc', imag_part, real_part, precision=highest)) / denominator
    out_re = jnp.einsum('cfp,fcb->bfp', real_part, gram_re, precision=highest) - jnp.einsum('cfp,fcb->bfp', imag_part, gram_im, precision=highest)
    out_im = jnp.einsum('cfp,fcb->bfp', real_part, gram_im, precision=highest) + jnp.einsum('cfp,fcb->bfp', imag_part, gram_re, precision=highest)
    power = jnp.stack([out_re, out_im], axis=1)
    spectra_out = spectra.reshape(NB, 2, NF, GROUPS, GROUP_PTS).transpose(3, 0, 1, 2, 4)
    power_out = power.reshape(NB, 2, NF, GROUPS, GROUP_PTS).transpose(3, 0, 1, 2, 4)
    return (spectra_out, power_out)
```

```python
import functools
import math

import jax
import jax.numpy as jnp
from jax import lax
from jax.experimental import pallas as pl
from jax.experimental.pallas import tpu as pltpu
from jax.sharding import Mesh
from jax.sharding import PartitionSpec as P

NFFT = 256
NB = 7
NF = 32
HALF = NB * NF
ROWS = 2 * HALF
TA = ("y", "zh", "x", "c")
F32 = jnp.float32
BF16 = jnp.bfloat16


def weights(block_starts, kept_freqs, times):
    offset = times[None, :] - block_starts[:, None]
    inside = (offset >= 0) & (offset < NFFT)
    window = 0.5 - 0.5 * jnp.cos(2.0 * math.pi / NFFT * offset.astype(F32))
    scale = jnp.where(inside, window, 0.0)
    phase = kept_freqs[None, :, None] * jnp.where(inside, offset, 0)[:, None, :] % NFFT
    angle = 2.0 * math.pi / NFFT * phase.astype(F32)
    norm = 2.0 / math.sqrt(NFFT)
    real = scale[:, None, :] * jnp.cos(angle) * norm
    imag = -scale[:, None, :] * jnp.sin(angle) * norm
    table = jnp.stack([real, imag]).astype(BF16)
    return table.reshape(ROWS, times.shape[0])


def same_freq(rows):
    row = lax.broadcasted_iota(jnp.int32, (rows, HALF), 0)
    col = lax.broadcasted_iota(jnp.int32, (rows, HALF), 1)
    return row % NF == col % NF


def dot(a, b):
    return jnp.dot(a, b, preferred_element_type=F32)


def dot_t(a, b):
    return lax.dot_general(a, b, (((1,), (1,)), ((), ())), preferred_element_type=F32)


def spectra_kernel(steps, w_ref, x_ref, s_ref, h_ref, acc):
    step = pl.program_id(0)
    parts = dot(w_ref[...], x_ref[...]).astype(BF16)
    for part in range(2):
        for b in range(NB):
            start = part * HALF + b * NF
            s_ref[b * 2 * NF + part * NF : b * 2 * NF + (part + 1) * NF, :] = parts[start : start + NF]
    real, imag = parts[:HALF], parts[HALF:]
    gram = dot_t(parts, real) + dot_t(jnp.concatenate([imag, -real], axis=0), imag)

    @pl.when(step == 0)
    def _():
        acc[...] = gram

    @pl.when(step > 0)
    def _():
        acc[...] += gram

    @pl.when(step == steps - 1)
    def _():
        kept = jnp.where(same_freq(ROWS), acc[...], 0.0)
        h_ref[...] = jnp.zeros_like(h_ref)
        h_ref[0 : 2 * NB, 0:HALF] = kept.reshape(2 * NB, NF, HALF).sum(axis=1)


def spectra_and_gram(w, x, width):
    times, pts = x.shape
    steps = pts // width
    return pl.pallas_call(
        functools.partial(spectra_kernel, steps),
        grid=(steps,),
        out_shape=(jax.ShapeDtypeStruct((ROWS, pts), BF16), jax.ShapeDtypeStruct((16, 256), F32)),
        in_specs=[
            pl.BlockSpec((ROWS, times), lambda i: (0, 0)),
            pl.BlockSpec((times, width), lambda i: (0, i)),
        ],
        out_specs=(pl.BlockSpec((ROWS, width), lambda i: (0, i)), pl.BlockSpec((16, 256), lambda i: (0, 0))),
        scratch_shapes=[pltpu.VMEM((ROWS, HALF), F32)],
        compiler_params=pltpu.CompilerParams(dimension_semantics=("arbitrary",), vmem_limit_bytes=40 * 2**20),
        cost_estimate=pl.CostEstimate(flops=2 * ROWS * times * pts, bytes_accessed=2 * times * pts, transcendentals=0),
        name="spectra",
    )(w, x)


def power_kernel(denominator, h_ref, s_ref, o_ref, m_ref):
    @pl.when(pl.program_id(0) == 0)
    def _():
        same = same_freq(NF)
        gram = h_ref[...] / denominator
        for b in range(NB):
            re = jnp.where(same, jnp.broadcast_to(gram[b : b + 1, :HALF], (NF, HALF)), 0.0)
            im = jnp.where(same, jnp.broadcast_to(gram[NB + b : NB + b + 1, :HALF], (NF, HALF)), 0.0)
            at = b * 2 * NF
            for part, (on_real, on_imag) in enumerate(((re, -im), (im, re))):
                for side, block in enumerate((on_real, on_imag)):
                    high = block.astype(BF16)
                    rows = slice(at + part * NF, at + (part + 1) * NF)
                    m_ref[2 * side, rows, :] = high
                    m_ref[2 * side + 1, rows, :] = (block - high.astype(F32)).astype(BF16)

    real = jnp.concatenate([s_ref[b * 2 * NF : b * 2 * NF + NF, :] for b in range(NB)], axis=0)
    imag = jnp.concatenate([s_ref[b * 2 * NF + NF : (b + 1) * 2 * NF, :] for b in range(NB)], axis=0)
    low = dot(m_ref[1], real) + dot(m_ref[3], imag)
    o_ref[...] = low + dot(m_ref[0], real) + dot(m_ref[2], imag)


def power(h, s, denominator, width):
    pts = s.shape[1]
    return pl.pallas_call(
        functools.partial(power_kernel, denominator),
        grid=(pts // width,),
        out_shape=jax.ShapeDtypeStruct((ROWS, pts), F32),
        in_specs=[pl.BlockSpec((16, 256), lambda i: (0, 0)), pl.BlockSpec((ROWS, width), lambda i: (0, i))],
        out_specs=pl.BlockSpec((ROWS, width), lambda i: (0, i)),
        scratch_shapes=[pltpu.VMEM((4, ROWS, HALF), BF16)],
        compiler_params=pltpu.CompilerParams(dimension_semantics=("arbitrary",), vmem_limit_bytes=40 * 2**20),
        name="power",
    )(h, s)


def sum_over(h, axes):
    count = lax.axis_size(axes)
    copies = jnp.broadcast_to(h[None], (count, *h.shape))
    return lax.all_to_all(copies, axes, 0, 0, tiled=True).sum(axis=0)


def shards(snapshots, block_starts, kept_freqs):
    count = lax.axis_size(TA)
    local = snapshots.shape[0]
    own = snapshots.shape[2] // count
    total = own * count * lax.axis_size("zl")
    blocks = snapshots.reshape(local, count, own).transpose(1, 0, 2)
    arrived = lax.all_to_all(blocks, TA, split_axis=0, concat_axis=0, tiled=True)
    w = weights(block_starts, kept_freqs, jnp.arange(local * count, dtype=jnp.int32))
    s, h = spectra_and_gram(w, arrived.reshape(local * count, own), 512)
    h = sum_over(h, ("y", "x"))
    h = sum_over(h, ("zh", "zl", "c"))
    out = power(h, s, float(NB * total), 512)
    shape = (1, NB, 2, NF, own)
    return s.reshape(shape), out.reshape(shape)


def solution(mesh):
    split = Mesh(mesh.devices.reshape(4, 2, 4, 2, mesh.shape["ga"]), ("y", "zh", "x", "c", "zl"))
    out = P("zl", None, None, None, TA)
    return jax.shard_map(
        shards, mesh=split, in_specs=(P(TA, "zl", None), P(), P()), out_specs=(out, out), check_vma=False
    )
```

```python
import functools
import math

import jax
import jax.numpy as jnp
from jax import lax
from jax.experimental import pallas as pl
from jax.experimental.pallas import tpu as pltpu
from jax.sharding import Mesh
from jax.sharding import PartitionSpec as P


NFFT = 256
NB = 7
NF = 32
HALF = NB * NF
ROWS = 2 * HALF
PAIRS = NB // 2
TA = ("y", "zh", "x", "c")
PLANE = ("y", "x", "c")
FIRST = 1024
WIDTH = 512
F32 = jnp.float32
BF16 = jnp.bfloat16
PARAMS = pltpu.CompilerParams(dimension_semantics=("arbitrary",), vmem_limit_bytes=60 * 2**20)


def weights(block_starts, kept_freqs, times):
    offset = times[None, :] - block_starts[:, None]
    inside = (offset >= 0) & (offset < NFFT)
    window = 0.5 - 0.5 * jnp.cos(2.0 * math.pi / NFFT * offset.astype(F32))
    scale = jnp.where(inside, window, 0.0)
    phase = kept_freqs[None, :, None] * jnp.where(inside, offset, 0)[:, None, :] % NFFT
    angle = 2.0 * math.pi / NFFT * phase.astype(F32)
    norm = 2.0 / math.sqrt(NFFT)
    real = scale[:, None, :] * jnp.cos(angle) * norm
    imag = -scale[:, None, :] * jnp.sin(angle) * norm
    table = jnp.stack([real, imag]).astype(BF16)
    return table.reshape(ROWS, times.shape[0])


def dot(a, b):
    return jnp.dot(a, b, preferred_element_type=F32)


def dot_t(a, b):
    return lax.dot_general(a, b, (((1,), (1,)), ((), ())), preferred_element_type=F32)


def same_freq(rows):
    row = lax.broadcasted_iota(jnp.int32, (rows, HALF), 0)
    col = lax.broadcasted_iota(jnp.int32, (rows, HALF), 1)
    return row % NF == col % NF


def pack_kernel(own, jobs, x_ref, *refs):
    outs, sems = refs[:-1], refs[-1]
    me = lax.axis_index("zh")
    copies = []
    for out, (shift, low) in zip(outs, jobs):
        side = (me + shift) % 2
        for d in range(out.shape[0]):
            start = ((d // 8) * 16 + d % 8) * own + low + side * (8 * own)
            cols = pl.ds(pl.multiple_of(start, 128), out.shape[2])
            copies.append(pltpu.make_async_copy(x_ref.at[:, cols], out.at[d], sems.at[len(copies)]))
    for copy in copies:
        copy.start()
    for copy in copies:
        copy.wait()


def pack(x, own, jobs):
    count = x.shape[1] // own // 2
    shapes = [jax.ShapeDtypeStruct((count, x.shape[0], n), x.dtype) for _, _, n in jobs]
    return pl.pallas_call(
        functools.partial(pack_kernel, own, [job[:2] for job in jobs]),
        out_shape=shapes,
        in_specs=[pl.BlockSpec(memory_space=pltpu.HBM)],
        out_specs=[pl.BlockSpec(memory_space=pltpu.VMEM)] * len(jobs),
        scratch_shapes=[pltpu.SemaphoreType.DMA((count * len(jobs),))],
        compiler_params=pltpu.CompilerParams(vmem_limit_bytes=60 * 2**20),
        name="pack",
    )(x)


def emit(parts, s_ref):
    for part in range(2):
        for b in range(NB):
            start = part * HALF + b * NF
            s_ref[b * 2 * NF + part * NF : b * 2 * NF + (part + 1) * NF, :] = parts[start : start + NF]


def gram_of(parts):
    real, imag = parts[:HALF], parts[HALF:]
    return dot_t(parts, real) + dot_t(jnp.concatenate([imag, -real], axis=0), imag)


def rows_of(ref):
    return ref[...].reshape(-1, ref.shape[2])


def whole_kernel(w0_ref, w1_ref, x0_ref, x1_ref, s_ref, g_ref):
    parts = (dot(w0_ref[...], rows_of(x0_ref)) + dot(w1_ref[...], rows_of(x1_ref))).astype(BF16)
    emit(parts, s_ref)
    gram = gram_of(parts)

    @pl.when(pl.program_id(0) == 0)
    def _():
        g_ref[...] = gram

    @pl.when(pl.program_id(0) > 0)
    def _():
        g_ref[...] += gram


def whole(w0, w1, x0, x1, pts):
    times = w0.shape[1]
    steps = x1.shape[2] // WIDTH
    fixed = pl.BlockSpec((ROWS, times), lambda i: (0, 0))
    moving = pl.BlockSpec((*x0.shape[:2], WIDTH), lambda i: (0, 0, i))
    return pl.pallas_call(
        whole_kernel,
        grid=(steps,),
        out_shape=(jax.ShapeDtypeStruct((ROWS, pts), BF16), jax.ShapeDtypeStruct((ROWS, HALF), F32)),
        in_specs=[fixed, fixed, moving, moving],
        out_specs=(pl.BlockSpec((ROWS, WIDTH), lambda i: (0, i)), pl.BlockSpec((ROWS, HALF), lambda i: (0, 0))),
        compiler_params=PARAMS,
        cost_estimate=pl.CostEstimate(flops=4 * ROWS * times * steps * WIDTH, bytes_accessed=2**22, transcendentals=0),
        name="whole",
    )(w0, w1, x0, x1)


def partial_kernel(w_ref, x_ref, p_ref):
    p_ref[...] = dot(w_ref[...], rows_of(x_ref))


def partial(w, x, first):
    times = w.shape[1]
    pts = x.shape[2] - first
    skip = first // WIDTH
    return pl.pallas_call(
        partial_kernel,
        grid=(pts // WIDTH,),
        out_shape=jax.ShapeDtypeStruct((ROWS, pts), F32),
        in_specs=[
            pl.BlockSpec((ROWS, times), lambda i: (0, 0)),
            pl.BlockSpec((*x.shape[:2], WIDTH), lambda i: (0, 0, i + skip)),
        ],
        out_specs=pl.BlockSpec((ROWS, WIDTH), lambda i: (0, i)),
        compiler_params=PARAMS,
        cost_estimate=pl.CostEstimate(flops=2 * ROWS * times * pts, bytes_accessed=2**21, transcendentals=0),
        name="partial",
    )(w, x)


def lane_block(rows):
    return lax.broadcasted_iota(jnp.int32, (rows, HALF), 1) // NF


def rest_kernel(steps, w_ref, x_ref, p_ref, g_ref, _, s_ref, t_ref, acc):
    step = pl.program_id(0)
    parts = (p_ref[...] + dot(w_ref[...], rows_of(x_ref))).astype(BF16)
    emit(parts, s_ref)
    gram = gram_of(parts)

    @pl.when(step == 0)
    def _():
        acc[...] = g_ref[...] + gram

    @pl.when(step > 0)
    def _():
        acc[...] += gram

    @pl.when(step == steps - 1)
    def _():
        kept = jnp.where(same_freq(ROWS), acc[...], 0.0)
        tables = kept.reshape(2 * NB, NF, HALF).sum(axis=1)
        block = lax.broadcasted_iota(jnp.int32, (NB, HALF), 0)
        t_ref[...] = jnp.zeros_like(t_ref)
        for k in range(PAIRS + 1):
            pick = (lane_block(NB) + k) % NB == block
            t_ref[k : k + 1, :HALF] = jnp.where(pick, tables[:NB], 0.0).sum(axis=0, keepdims=True)
            if k:
                row = PAIRS + k
                t_ref[row : row + 1, :HALF] = jnp.where(pick, tables[NB:], 0.0).sum(axis=0, keepdims=True)


def rest(w, x, p, g, s):
    times = w.shape[1]
    steps = x.shape[2] // WIDTH
    skip = s.shape[1] // WIDTH - steps
    return pl.pallas_call(
        functools.partial(rest_kernel, steps),
        grid=(steps,),
        out_shape=(jax.ShapeDtypeStruct(s.shape, BF16), jax.ShapeDtypeStruct((8, 256), F32)),
        in_specs=[
            pl.BlockSpec((ROWS, times), lambda i: (0, 0)),
            pl.BlockSpec((*x.shape[:2], WIDTH), lambda i: (0, 0, i)),
            pl.BlockSpec((ROWS, WIDTH), lambda i: (0, i)),
            pl.BlockSpec((ROWS, HALF), lambda i: (0, 0)),
            pl.BlockSpec(memory_space=pl.ANY),
        ],
        out_specs=(pl.BlockSpec((ROWS, WIDTH), lambda i: (0, i + skip)), pl.BlockSpec((8, 256), lambda i: (0, 0))),
        scratch_shapes=[pltpu.VMEM((ROWS, HALF), F32)],
        input_output_aliases={4: 0},
        compiler_params=PARAMS,
        cost_estimate=pl.CostEstimate(flops=2 * ROWS * times * steps * WIDTH, bytes_accessed=2**22, transcendentals=0),
        name="rest",
    )(w, x, p, g, s)


def turned(row, k):
    lane = lax.broadcasted_iota(jnp.int32, row.shape, 1)
    near = pltpu.roll(row, 256 - k * NF, 1)
    far = pltpu.roll(row, HALF - k * NF, 1)
    return jnp.where(lane < HALF - k * NF, near, far)


def power_kernel(denominator, t_ref, s_ref, o_ref, m_ref):
    @pl.when(pl.program_id(0) == 0)
    def _():
        sums = jnp.sum(t_ref[...], axis=0) / denominator
        real_rows = [sums[k : k + 1, :] for k in range(PAIRS + 1)]
        imag_rows = [jnp.zeros_like(real_rows[0])] + [sums[PAIRS + k : PAIRS + k + 1, :] for k in range(1, PAIRS + 1)]
        for k in range(PAIRS + 1, NB):
            real_rows.append(turned(real_rows[NB - k], k))
            imag_rows.append(-turned(imag_rows[NB - k], k))
        same = same_freq(NF)
        block = lane_block(1)
        for b in range(NB):
            re = sum(jnp.where((block + k) % NB == b, real_rows[k][:, :HALF], 0.0) for k in range(NB))
            im = sum(jnp.where((block + k) % NB == b, imag_rows[k][:, :HALF], 0.0) for k in range(NB))
            re = jnp.where(same, jnp.broadcast_to(re, (NF, HALF)), 0.0)
            im = jnp.where(same, jnp.broadcast_to(im, (NF, HALF)), 0.0)
            at = b * 2 * NF
            for part, (on_real, on_imag) in enumerate(((re, -im), (im, re))):
                for side, value in enumerate((on_real, on_imag)):
                    high = value.astype(BF16)
                    rows = slice(at + part * NF, at + (part + 1) * NF)
                    m_ref[2 * side, rows, :] = high
                    m_ref[2 * side + 1, rows, :] = (value - high.astype(F32)).astype(BF16)

    real = jnp.concatenate([s_ref[b * 2 * NF : b * 2 * NF + NF, :] for b in range(NB)], axis=0)
    imag = jnp.concatenate([s_ref[b * 2 * NF + NF : (b + 1) * 2 * NF, :] for b in range(NB)], axis=0)
    low = dot(m_ref[1], real) + dot(m_ref[3], imag)
    o_ref[...] = low + dot(m_ref[0], real) + dot(m_ref[2], imag)


def power(t, s, denominator):
    pts = s.shape[1]
    return pl.pallas_call(
        functools.partial(power_kernel, denominator),
        grid=(pts // WIDTH,),
        out_shape=jax.ShapeDtypeStruct((ROWS, pts), F32),
        in_specs=[
            pl.BlockSpec(t.shape, lambda i: (0, 0, 0)),
            pl.BlockSpec((ROWS, WIDTH), lambda i: (0, i)),
        ],
        out_specs=pl.BlockSpec((ROWS, WIDTH), lambda i: (0, i)),
        scratch_shapes=[pltpu.VMEM((4, ROWS, HALF), BF16)],
        compiler_params=PARAMS,
        name="power",
    )(t, s)


def to_all(t, axes):
    copies = jnp.broadcast_to(t[None], (lax.axis_size(axes), *t.shape))
    return lax.all_to_all(copies, axes, 0, 0, tiled=True)


def exchange(x, axes):
    return lax.all_to_all(x, axes, 0, 0, tiled=True)


def shards(snapshots, block_starts, kept_freqs):
    count = lax.axis_size(TA)
    local = snapshots.shape[0]
    own = snapshots.shape[2] // count
    total = own * count * lax.axis_size("zl")
    swap = [(0, 1), (1, 0)]
    x = snapshots.reshape(local, own * count)

    (first_out,) = pack(x, own, [(1, 0, FIRST)])
    first_in = lax.ppermute(first_out, "zh", swap)
    pass_on, mine = pack(x, own, [(1, FIRST, own - FIRST), (0, 0, own)])
    pass_on = exchange(pass_on, PLANE)
    side = lax.axis_index("zh")
    place = jnp.arange(local * count // 2, dtype=jnp.int32)
    times = place // 128 * 256 + place % 128
    w0 = weights(block_starts, kept_freqs, times + side * 128)
    w1 = weights(block_starts, kept_freqs, times + (1 - side) * 128)
    pass_on, w0, w1 = lax.optimization_barrier((pass_on, w0, w1))
    rest_in = lax.ppermute(pass_on, "zh", swap)
    x0 = exchange(mine, PLANE)
    x1 = exchange(first_in, PLANE)
    s, g = whole(w0, w1, x0, x1, own)
    p = partial(w0, x0, FIRST)
    s, t = rest(w1, rest_in, p, g, s)
    t = to_all(t, ("y", "x")).sum(axis=0)
    t = to_all(t, ("zh", "zl", "c"))
    out = power(t, s, float(NB * total))
    shape = (1, NB, 2, NF, own)
    return s.reshape(shape), out.reshape(shape)


def solution(mesh):
    split = Mesh(mesh.devices.reshape(4, 2, 4, 2, mesh.shape["ga"]), ("y", "zh", "x", "c", "zl"))
    out = P("zl", None, None, None, TA)
    return jax.shard_map(
        shards, mesh=split, in_specs=(P(TA, "zl", None), P(), P()), out_specs=(out, out), check_vma=False
    )
```

```python
import functools
import math

import jax
import jax.numpy as jnp
from jax import lax
from jax.experimental import pallas as pl
from jax.experimental.pallas import tpu as pltpu
from jax.sharding import Mesh
from jax.sharding import PartitionSpec as P


NFFT = 256
NB = 7
NF = 32
HALF = NB * NF
ROWS = 2 * HALF
PAIRS = NB // 2
TA = ("y", "zh", "x", "c")
PLANE = ("y", "x", "c")
FIRST = 512
EACH = 768
WIDTH = 512
F32 = jnp.float32
BF16 = jnp.bfloat16
PARAMS = pltpu.CompilerParams(dimension_semantics=("arbitrary",), vmem_limit_bytes=60 * 2**20)


def weights(block_starts, kept_freqs, times):
    offset = times[None, :] - block_starts[:, None]
    inside = (offset >= 0) & (offset < NFFT)
    window = 0.5 - 0.5 * jnp.cos(2.0 * math.pi / NFFT * offset.astype(F32))
    scale = jnp.where(inside, window, 0.0)
    phase = kept_freqs[None, :, None] * jnp.where(inside, offset, 0)[:, None, :] % NFFT
    angle = 2.0 * math.pi / NFFT * phase.astype(F32)
    norm = 2.0 / math.sqrt(NFFT)
    real = scale[:, None, :] * jnp.cos(angle) * norm
    imag = -scale[:, None, :] * jnp.sin(angle) * norm
    table = jnp.stack([real, imag]).astype(BF16)
    return table.reshape(ROWS, times.shape[0])


def dot(a, b):
    return jnp.dot(a, b, preferred_element_type=F32)


def dot_t(a, b):
    return lax.dot_general(a, b, (((1,), (1,)), ((), ())), preferred_element_type=F32)


def same_freq(rows):
    row = lax.broadcasted_iota(jnp.int32, (rows, HALF), 0)
    col = lax.broadcasted_iota(jnp.int32, (rows, HALF), 1)
    return row % NF == col % NF


def pack_kernel(own, jobs, x_ref, *refs):
    outs, sems = refs[:-1], refs[-1]
    me = lax.axis_index("zh")
    copies = []
    for out, (shift, low) in zip(outs, jobs):
        side = (me + shift) % 2
        for d in range(out.shape[0]):
            start = ((d // 8) * 16 + d % 8) * own + low + side * (8 * own)
            cols = pl.ds(pl.multiple_of(start, 128), out.shape[2])
            copies.append(pltpu.make_async_copy(x_ref.at[:, cols], out.at[d], sems.at[len(copies)]))
    for copy in copies:
        copy.start()
    for copy in copies:
        copy.wait()


def pack(x, own, jobs):
    count = x.shape[1] // own // 2
    shapes = [jax.ShapeDtypeStruct((count, x.shape[0], n), x.dtype) for _, _, n in jobs]
    return pl.pallas_call(
        functools.partial(pack_kernel, own, [job[:2] for job in jobs]),
        out_shape=shapes,
        in_specs=[pl.BlockSpec(memory_space=pltpu.HBM)],
        out_specs=[pl.BlockSpec(memory_space=pltpu.VMEM)] * len(jobs),
        scratch_shapes=[pltpu.SemaphoreType.DMA((count * len(jobs),))],
        compiler_params=pltpu.CompilerParams(vmem_limit_bytes=60 * 2**20),
        name="pack",
    )(x)


def emit(parts, s_ref):
    for part in range(2):
        for b in range(NB):
            start = part * HALF + b * NF
            s_ref[b * 2 * NF + part * NF : b * 2 * NF + (part + 1) * NF, :] = parts[start : start + NF]


def gram_of(parts):
    real, imag = parts[:HALF], parts[HALF:]
    return dot_t(parts, real) + dot_t(jnp.concatenate([imag, -real], axis=0), imag)


def rows_of(ref):
    return ref[...].reshape(-1, ref.shape[2])


def whole_kernel(w0_ref, w1_ref, x0_ref, x1_ref, s_ref, g_ref):
    parts = (dot(w0_ref[...], rows_of(x0_ref)) + dot(w1_ref[...], rows_of(x1_ref))).astype(BF16)
    emit(parts, s_ref)
    g_ref[...] = gram_of(parts)


def whole(w0, w1, x0, x1):
    times = w0.shape[1]
    pts, count = x0.shape[2], x1.shape[2]
    at = pts // count - 1
    fixed = pl.BlockSpec((ROWS, times), lambda i: (0, 0))
    return pl.pallas_call(
        whole_kernel,
        grid=(1,),
        out_shape=(jax.ShapeDtypeStruct((ROWS, pts), BF16), jax.ShapeDtypeStruct((ROWS, HALF), F32)),
        in_specs=[
            fixed,
            fixed,
            pl.BlockSpec((*x0.shape[:2], count), lambda i: (0, 0, at)),
            pl.BlockSpec(x1.shape, lambda i: (0, 0, 0)),
        ],
        out_specs=(pl.BlockSpec((ROWS, count), lambda i: (0, at)), pl.BlockSpec((ROWS, HALF), lambda i: (0, 0))),
        compiler_params=PARAMS,
        cost_estimate=pl.CostEstimate(flops=4 * ROWS * times * count, bytes_accessed=2**22, transcendentals=0),
        name="whole",
    )(w0, w1, x0, x1)


def partial_kernel(w_ref, x_ref, p_ref):
    p_ref[...] = dot(w_ref[...], rows_of(x_ref))


def partial(w, x, pts):
    times = w.shape[1]
    width = EACH // 2
    return pl.pallas_call(
        partial_kernel,
        grid=(pts // width,),
        out_shape=jax.ShapeDtypeStruct((ROWS, pts), F32),
        in_specs=[
            pl.BlockSpec((ROWS, times), lambda i: (0, 0)),
            pl.BlockSpec((*x.shape[:2], width), lambda i: (0, 0, i)),
        ],
        out_specs=pl.BlockSpec((ROWS, width), lambda i: (0, i)),
        compiler_params=PARAMS,
        cost_estimate=pl.CostEstimate(flops=2 * ROWS * times * pts, bytes_accessed=2**21, transcendentals=0),
        name="partial",
    )(w, x)


def lane_block(rows):
    return lax.broadcasted_iota(jnp.int32, (rows, HALF), 1) // NF


def next_kernel(w_ref, x_ref, p_ref, g_ref, _, s_ref, out_ref, last):
    parts = (p_ref[...] + dot(w_ref[...], rows_of(x_ref))).astype(BF16)
    emit(parts, s_ref)
    total = g_ref[...] + gram_of(parts)
    if not last:
        out_ref[...] = total
        return
    kept = jnp.where(same_freq(ROWS), total, 0.0)
    tables = kept.reshape(2 * NB, NF, HALF).sum(axis=1)
    block = lax.broadcasted_iota(jnp.int32, (NB, HALF), 0)
    out_ref[...] = jnp.zeros_like(out_ref)
    for k in range(PAIRS + 1):
        pick = (lane_block(NB) + k) % NB == block
        out_ref[k : k + 1, :HALF] = jnp.where(pick, tables[:NB], 0.0).sum(axis=0, keepdims=True)
        if k:
            row = PAIRS + k
            out_ref[row : row + 1, :HALF] = jnp.where(pick, tables[NB:], 0.0).sum(axis=0, keepdims=True)


def next_part(at, last, w, x, p, g, s):
    times = w.shape[1]
    width = x.shape[2]
    out = (8, 256) if last else (ROWS, HALF)
    return pl.pallas_call(
        functools.partial(next_kernel, last=last),
        grid=(1,),
        out_shape=(jax.ShapeDtypeStruct(s.shape, BF16), jax.ShapeDtypeStruct(out, F32)),
        in_specs=[
            pl.BlockSpec((ROWS, times), lambda i: (0, 0)),
            pl.BlockSpec(x.shape, lambda i: (0, 0, 0)),
            pl.BlockSpec((ROWS, width), lambda i: (0, at)),
            pl.BlockSpec((ROWS, HALF), lambda i: (0, 0)),
            pl.BlockSpec(memory_space=pl.ANY),
        ],
        out_specs=(pl.BlockSpec((ROWS, width), lambda i: (0, at)), pl.BlockSpec(out, lambda i: (0, 0))),
        input_output_aliases={4: 0},
        compiler_params=PARAMS,
        cost_estimate=pl.CostEstimate(flops=2 * ROWS * times * width, bytes_accessed=2**22, transcendentals=0),
        name="next_part",
    )(w, x, p, g, s)


def turned(row, k):
    lane = lax.broadcasted_iota(jnp.int32, row.shape, 1)
    near = pltpu.roll(row, 256 - k * NF, 1)
    far = pltpu.roll(row, HALF - k * NF, 1)
    return jnp.where(lane < HALF - k * NF, near, far)


def power_kernel(denominator, t_ref, s_ref, o_ref, m_ref):
    @pl.when(pl.program_id(0) == 0)
    def _():
        sums = jnp.sum(t_ref[...], axis=0) / denominator
        real_rows = [sums[k : k + 1, :] for k in range(PAIRS + 1)]
        imag_rows = [jnp.zeros_like(real_rows[0])] + [sums[PAIRS + k : PAIRS + k + 1, :] for k in range(1, PAIRS + 1)]
        for k in range(PAIRS + 1, NB):
            real_rows.append(turned(real_rows[NB - k], k))
            imag_rows.append(-turned(imag_rows[NB - k], k))
        same = same_freq(NF)
        block = lane_block(1)
        for b in range(NB):
            re = sum(jnp.where((block + k) % NB == b, real_rows[k][:, :HALF], 0.0) for k in range(NB))
            im = sum(jnp.where((block + k) % NB == b, imag_rows[k][:, :HALF], 0.0) for k in range(NB))
            re = jnp.where(same, jnp.broadcast_to(re, (NF, HALF)), 0.0)
            im = jnp.where(same, jnp.broadcast_to(im, (NF, HALF)), 0.0)
            at = b * 2 * NF
            for part, (on_real, on_imag) in enumerate(((re, -im), (im, re))):
                for side, value in enumerate((on_real, on_imag)):
                    high = value.astype(BF16)
                    rows = slice(at + part * NF, at + (part + 1) * NF)
                    m_ref[2 * side, rows, :] = high
                    m_ref[2 * side + 1, rows, :] = (value - high.astype(F32)).astype(BF16)

    real = jnp.concatenate([s_ref[b * 2 * NF : b * 2 * NF + NF, :] for b in range(NB)], axis=0)
    imag = jnp.concatenate([s_ref[b * 2 * NF + NF : (b + 1) * 2 * NF, :] for b in range(NB)], axis=0)
    low = dot(m_ref[1], real) + dot(m_ref[3], imag)
    o_ref[...] = low + dot(m_ref[0], real) + dot(m_ref[2], imag)


def power(t, s, denominator):
    pts = s.shape[1]
    return pl.pallas_call(
        functools.partial(power_kernel, denominator),
        grid=(pts // WIDTH,),
        out_shape=jax.ShapeDtypeStruct((ROWS, pts), F32),
        in_specs=[
            pl.BlockSpec(t.shape, lambda i: (0, 0, 0)),
            pl.BlockSpec((ROWS, WIDTH), lambda i: (0, i)),
        ],
        out_specs=pl.BlockSpec((ROWS, WIDTH), lambda i: (0, i)),
        scratch_shapes=[pltpu.VMEM((4, ROWS, HALF), BF16)],
        compiler_params=PARAMS,
        name="power",
    )(t, s)


def to_all(t, axes):
    copies = jnp.broadcast_to(t[None], (lax.axis_size(axes), *t.shape))
    return lax.all_to_all(copies, axes, 0, 0, tiled=True)


def exchange(x, axes):
    return lax.all_to_all(x, axes, 0, 0, tiled=True)


def shards(snapshots, block_starts, kept_freqs):
    count = lax.axis_size(TA)
    local = snapshots.shape[0]
    own = snapshots.shape[2] // count
    total = own * count * lax.axis_size("zl")
    swap = [(0, 1), (1, 0)]
    x = snapshots.reshape(local, own * count)

    later = own - FIRST
    (first,) = pack(x, own, [(1, later, FIRST)])
    first = lax.ppermute(first, "zh", swap)
    (part0,) = pack(x, own, [(1, 0, EACH)])
    part0 = exchange(part0, PLANE)
    part0 = lax.ppermute(part0, "zh", swap)
    part1, mine = pack(x, own, [(1, EACH, EACH), (0, 0, own)])
    part1 = exchange(part1, PLANE)
    x0 = exchange(mine, PLANE)
    side = lax.axis_index("zh")
    place = jnp.arange(local * count // 2, dtype=jnp.int32)
    times = place // 128 * 256 + place % 128
    w0 = weights(block_starts, kept_freqs, times + side * 128)
    w1 = weights(block_starts, kept_freqs, times + (1 - side) * 128)
    part1, w0, w1 = lax.optimization_barrier((part1, w0, w1))
    part1 = lax.ppermute(part1, "zh", swap)
    first = exchange(first, PLANE)
    p = partial(w0, x0, later)
    s, g = whole(w0, w1, x0, first)
    s, g = next_part(0, False, w1, part0, p, g, s)
    s, t = next_part(1, True, w1, part1, p, g, s)
    t = to_all(t, ("y", "x")).sum(axis=0)
    t = to_all(t, ("zh", "zl", "c"))
    out = power(t, s, float(NB * total))
    shape = (1, NB, 2, NF, own)
    return s.reshape(shape), out.reshape(shape)


def solution(mesh):
    split = Mesh(mesh.devices.reshape(4, 2, 4, 2, mesh.shape["ga"]), ("y", "zh", "x", "c", "zl"))
    out = P("zl", None, None, None, TA)
    return jax.shard_map(
        shards, mesh=split, in_specs=(P(TA, "zl", None), P(), P()), out_specs=(out, out), check_vma=False
    )
```

```python
import functools
import math

import jax
import jax.numpy as jnp
from jax import lax
from jax.experimental import pallas as pl
from jax.experimental.pallas import tpu as pltpu
from jax.sharding import Mesh
from jax.sharding import PartitionSpec as P


NFFT = 256
NB = 7
NF = 32
HALF = NB * NF
ROWS = 2 * HALF
PAIRS = NB // 2
TA = ("y", "zh", "x", "c")
PLANE = ("y", "x", "c")
FIRST = 768
WIDTH = 512
F32 = jnp.float32
BF16 = jnp.bfloat16
PARAMS = pltpu.CompilerParams(dimension_semantics=("arbitrary",), vmem_limit_bytes=60 * 2**20)


def weights(block_starts, kept_freqs, times):
    offset = times[None, :] - block_starts[:, None]
    inside = (offset >= 0) & (offset < NFFT)
    window = 0.5 - 0.5 * jnp.cos(2.0 * math.pi / NFFT * offset.astype(F32))
    scale = jnp.where(inside, window, 0.0)
    phase = kept_freqs[None, :, None] * jnp.where(inside, offset, 0)[:, None, :] % NFFT
    angle = 2.0 * math.pi / NFFT * phase.astype(F32)
    norm = 2.0 / math.sqrt(NFFT)
    real = scale[:, None, :] * jnp.cos(angle) * norm
    imag = -scale[:, None, :] * jnp.sin(angle) * norm
    table = jnp.stack([real, imag]).astype(BF16)
    return table.reshape(ROWS, times.shape[0])


def dot(a, b):
    return jnp.dot(a, b, preferred_element_type=F32)


def dot_t(a, b):
    return lax.dot_general(a, b, (((1,), (1,)), ((), ())), preferred_element_type=F32)


def same_freq(rows):
    row = lax.broadcasted_iota(jnp.int32, (rows, HALF), 0)
    col = lax.broadcasted_iota(jnp.int32, (rows, HALF), 1)
    return row % NF == col % NF


def pack_kernel(own, jobs, x_ref, *refs):
    outs, sems = refs[:-1], refs[-1]
    me = lax.axis_index("zh")
    copies = []
    for out, (shift, low) in zip(outs, jobs):
        side = (me + shift) % 2
        for d in range(out.shape[0]):
            start = ((d // 8) * 16 + d % 8) * own + low + side * (8 * own)
            cols = pl.ds(pl.multiple_of(start, 128), out.shape[2])
            copies.append(pltpu.make_async_copy(x_ref.at[:, cols], out.at[d], sems.at[len(copies)]))
    for copy in copies:
        copy.start()
    for copy in copies:
        copy.wait()


def pack(x, own, jobs):
    count = x.shape[1] // own // 2
    shapes = [jax.ShapeDtypeStruct((count, x.shape[0], n), x.dtype) for _, _, n in jobs]
    return pl.pallas_call(
        functools.partial(pack_kernel, own, [job[:2] for job in jobs]),
        out_shape=shapes,
        in_specs=[pl.BlockSpec(memory_space=pltpu.HBM)],
        out_specs=[pl.BlockSpec(memory_space=pltpu.VMEM)] * len(jobs),
        scratch_shapes=[pltpu.SemaphoreType.DMA((count * len(jobs),))],
        compiler_params=pltpu.CompilerParams(vmem_limit_bytes=60 * 2**20),
        name="pack",
    )(x)


def emit(parts, s_ref):
    for part in range(2):
        for b in range(NB):
            start = part * HALF + b * NF
            s_ref[b * 2 * NF + part * NF : b * 2 * NF + (part + 1) * NF, :] = parts[start : start + NF]


def gram_of(parts):
    real, imag = parts[:HALF], parts[HALF:]
    return dot_t(parts, real) + dot_t(jnp.concatenate([imag, -real], axis=0), imag)


def rows_of(ref):
    return ref[...].reshape(-1, ref.shape[2])


def whole_kernel(w0_ref, w1_ref, x0_ref, x1_ref, s_ref, g_ref):
    parts = (dot(w0_ref[...], rows_of(x0_ref)) + dot(w1_ref[...], rows_of(x1_ref))).astype(BF16)
    emit(parts, s_ref)
    gram = gram_of(parts)

    @pl.when(pl.program_id(0) == 0)
    def _():
        g_ref[...] = gram

    @pl.when(pl.program_id(0) > 0)
    def _():
        g_ref[...] += gram


def whole(w0, w1, x0, x1, width):
    times = w0.shape[1]
    pts, count = x0.shape[2], x1.shape[2]
    skip = (pts - count) // width
    fixed = pl.BlockSpec((ROWS, times), lambda i: (0, 0))
    return pl.pallas_call(
        whole_kernel,
        grid=(count // width,),
        out_shape=(jax.ShapeDtypeStruct((ROWS, pts), BF16), jax.ShapeDtypeStruct((ROWS, HALF), F32)),
        in_specs=[
            fixed,
            fixed,
            pl.BlockSpec((*x0.shape[:2], width), lambda i: (0, 0, i + skip)),
            pl.BlockSpec((*x0.shape[:2], width), lambda i: (0, 0, i)),
        ],
        out_specs=(pl.BlockSpec((ROWS, width), lambda i: (0, i + skip)), pl.BlockSpec((ROWS, HALF), lambda i: (0, 0))),
        compiler_params=PARAMS,
        cost_estimate=pl.CostEstimate(flops=4 * ROWS * times * count, bytes_accessed=2**22, transcendentals=0),
        name="whole",
    )(w0, w1, x0, x1)


def partial_kernel(w_ref, x_ref, p_ref):
    p_ref[...] = dot(w_ref[...], rows_of(x_ref))


def partial(w, x, pts, width):
    times = w.shape[1]
    return pl.pallas_call(
        partial_kernel,
        grid=(pts // width,),
        out_shape=jax.ShapeDtypeStruct((ROWS, pts), F32),
        in_specs=[
            pl.BlockSpec((ROWS, times), lambda i: (0, 0)),
            pl.BlockSpec((*x.shape[:2], width), lambda i: (0, 0, i)),
        ],
        out_specs=pl.BlockSpec((ROWS, width), lambda i: (0, i)),
        compiler_params=PARAMS,
        cost_estimate=pl.CostEstimate(flops=2 * ROWS * times * pts, bytes_accessed=2**21, transcendentals=0),
        name="partial",
    )(w, x)


def lane_block(rows):
    return lax.broadcasted_iota(jnp.int32, (rows, HALF), 1) // NF


def rest_kernel(steps, w_ref, x_ref, p_ref, g_ref, _, s_ref, t_ref, acc):
    step = pl.program_id(0)
    parts = (p_ref[...] + dot(w_ref[...], rows_of(x_ref))).astype(BF16)
    emit(parts, s_ref)
    gram = gram_of(parts)

    @pl.when(step == 0)
    def _():
        acc[...] = g_ref[...] + gram

    @pl.when(step > 0)
    def _():
        acc[...] += gram

    @pl.when(step == steps - 1)
    def _():
        kept = jnp.where(same_freq(ROWS), acc[...], 0.0)
        tables = kept.reshape(2 * NB, NF, HALF).sum(axis=1)
        block = lax.broadcasted_iota(jnp.int32, (NB, HALF), 0)
        t_ref[...] = jnp.zeros_like(t_ref)
        for k in range(PAIRS + 1):
            pick = (lane_block(NB) + k) % NB == block
            t_ref[k : k + 1, :HALF] = jnp.where(pick, tables[:NB], 0.0).sum(axis=0, keepdims=True)
            if k:
                row = PAIRS + k
                t_ref[row : row + 1, :HALF] = jnp.where(pick, tables[NB:], 0.0).sum(axis=0, keepdims=True)


def rest(w, x, p, g, s, width):
    times = w.shape[1]
    steps = x.shape[2] // width
    return pl.pallas_call(
        functools.partial(rest_kernel, steps),
        grid=(steps,),
        out_shape=(jax.ShapeDtypeStruct(s.shape, BF16), jax.ShapeDtypeStruct((8, 256), F32)),
        in_specs=[
            pl.BlockSpec((ROWS, times), lambda i: (0, 0)),
            pl.BlockSpec((*x.shape[:2], width), lambda i: (0, 0, i)),
            pl.BlockSpec((ROWS, width), lambda i: (0, i)),
            pl.BlockSpec((ROWS, HALF), lambda i: (0, 0)),
            pl.BlockSpec(memory_space=pl.ANY),
        ],
        out_specs=(pl.BlockSpec((ROWS, width), lambda i: (0, i)), pl.BlockSpec((8, 256), lambda i: (0, 0))),
        scratch_shapes=[pltpu.VMEM((ROWS, HALF), F32)],
        input_output_aliases={4: 0},
        compiler_params=PARAMS,
        cost_estimate=pl.CostEstimate(flops=2 * ROWS * times * x.shape[2], bytes_accessed=2**22, transcendentals=0),
        name="rest",
    )(w, x, p, g, s)


def turned(row, k):
    lane = lax.broadcasted_iota(jnp.int32, row.shape, 1)
    near = pltpu.roll(row, 256 - k * NF, 1)
    far = pltpu.roll(row, HALF - k * NF, 1)
    return jnp.where(lane < HALF - k * NF, near, far)


def power_kernel(denominator, t_ref, s_ref, o_ref, m_ref):
    @pl.when(pl.program_id(0) == 0)
    def _():
        sums = jnp.sum(t_ref[...], axis=0) / denominator
        real_rows = [sums[k : k + 1, :] for k in range(PAIRS + 1)]
        imag_rows = [jnp.zeros_like(real_rows[0])] + [sums[PAIRS + k : PAIRS + k + 1, :] for k in range(1, PAIRS + 1)]
        for k in range(PAIRS + 1, NB):
            real_rows.append(turned(real_rows[NB - k], k))
            imag_rows.append(-turned(imag_rows[NB - k], k))
        same = same_freq(NF)
        block = lane_block(1)
        for b in range(NB):
            re = sum(jnp.where((block + k) % NB == b, real_rows[k][:, :HALF], 0.0) for k in range(NB))
            im = sum(jnp.where((block + k) % NB == b, imag_rows[k][:, :HALF], 0.0) for k in range(NB))
            re = jnp.where(same, jnp.broadcast_to(re, (NF, HALF)), 0.0)
            im = jnp.where(same, jnp.broadcast_to(im, (NF, HALF)), 0.0)
            at = b * 2 * NF
            for part, (on_real, on_imag) in enumerate(((re, -im), (im, re))):
                for side, value in enumerate((on_real, on_imag)):
                    high = value.astype(BF16)
                    rows = slice(at + part * NF, at + (part + 1) * NF)
                    m_ref[2 * side, rows, :] = high
                    m_ref[2 * side + 1, rows, :] = (value - high.astype(F32)).astype(BF16)

    real = jnp.concatenate([s_ref[b * 2 * NF : b * 2 * NF + NF, :] for b in range(NB)], axis=0)
    imag = jnp.concatenate([s_ref[b * 2 * NF + NF : (b + 1) * 2 * NF, :] for b in range(NB)], axis=0)
    low = dot(m_ref[1], real) + dot(m_ref[3], imag)
    o_ref[...] = low + dot(m_ref[0], real) + dot(m_ref[2], imag)


def power(t, s, denominator):
    pts = s.shape[1]
    return pl.pallas_call(
        functools.partial(power_kernel, denominator),
        grid=(pts // WIDTH,),
        out_shape=jax.ShapeDtypeStruct((ROWS, pts), F32),
        in_specs=[
            pl.BlockSpec(t.shape, lambda i: (0, 0, 0)),
            pl.BlockSpec((ROWS, WIDTH), lambda i: (0, i)),
        ],
        out_specs=pl.BlockSpec((ROWS, WIDTH), lambda i: (0, i)),
        scratch_shapes=[pltpu.VMEM((4, ROWS, HALF), BF16)],
        compiler_params=PARAMS,
        name="power",
    )(t, s)


def to_all(t, axes):
    copies = jnp.broadcast_to(t[None], (lax.axis_size(axes), *t.shape))
    return lax.all_to_all(copies, axes, 0, 0, tiled=True)


def exchange(x, axes):
    return lax.all_to_all(x, axes, 0, 0, tiled=True)


def shards(snapshots, block_starts, kept_freqs):
    count = lax.axis_size(TA)
    local = snapshots.shape[0]
    own = snapshots.shape[2] // count
    total = own * count * lax.axis_size("zl")
    swap = [(0, 1), (1, 0)]
    x = snapshots.reshape(local, own * count)

    later = own - FIRST
    (first,) = pack(x, own, [(1, later, FIRST)])
    first = lax.ppermute(first, "zh", swap)
    (pass_on,) = pack(x, own, [(1, 0, later)])
    pass_on = exchange(pass_on, PLANE)
    passed = lax.ppermute(pass_on, "zh", swap)
    (mine,) = pack(x, own, [(0, 0, own)])
    x0 = exchange(mine, PLANE)
    side = lax.axis_index("zh")
    place = jnp.arange(local * count // 2, dtype=jnp.int32)
    times = place // 128 * 256 + place % 128
    w0 = weights(block_starts, kept_freqs, times + side * 128)
    w1 = weights(block_starts, kept_freqs, times + (1 - side) * 128)
    first, w0, w1 = lax.optimization_barrier((first, w0, w1))
    first = exchange(first, PLANE)
    p = partial(w0, x0, later, 640)
    s, g = whole(w0, w1, x0, first, 256)
    s, t = rest(w1, passed, p, g, s, 640)
    t = to_all(t, ("y", "x")).sum(axis=0)
    t = to_all(t, ("zh", "zl", "c"))
    out = power(t, s, float(NB * total))
    shape = (1, NB, 2, NF, own)
    return s.reshape(shape), out.reshape(shape)


def solution(mesh):
    split = Mesh(mesh.devices.reshape(4, 2, 4, 2, mesh.shape["ga"]), ("y", "zh", "x", "c", "zl"))
    out = P("zl", None, None, None, TA)
    return jax.shard_map(
        shards, mesh=split, in_specs=(P(TA, "zl", None), P(), P()), out_specs=(out, out), check_vma=False
    )
```

```python
import functools
import math

import jax
import jax.numpy as jnp
from jax import lax
from jax.experimental import pallas as pl
from jax.experimental.pallas import tpu as pltpu
from jax.sharding import Mesh
from jax.sharding import PartitionSpec as P


NFFT = 256
NB = 7
NF = 32
HALF = NB * NF
ROWS = 2 * HALF
PAIRS = NB // 2
TA = ("y", "zh", "x", "c")
PLANE = ("y", "x", "c")
FIRST = 768
WIDTH = 512
F32 = jnp.float32
BF16 = jnp.bfloat16
PARAMS = pltpu.CompilerParams(dimension_semantics=("arbitrary",), vmem_limit_bytes=60 * 2**20)


def weights(block_starts, kept_freqs, times):
    offset = times[None, :] - block_starts[:, None]
    inside = (offset >= 0) & (offset < NFFT)
    window = 0.5 - 0.5 * jnp.cos(2.0 * math.pi / NFFT * offset.astype(F32))
    scale = jnp.where(inside, window, 0.0)
    phase = kept_freqs[None, :, None] * jnp.where(inside, offset, 0)[:, None, :] % NFFT
    angle = 2.0 * math.pi / NFFT * phase.astype(F32)
    norm = 2.0 / math.sqrt(NFFT)
    real = scale[:, None, :] * jnp.cos(angle) * norm
    imag = -scale[:, None, :] * jnp.sin(angle) * norm
    table = jnp.stack([real, imag]).astype(BF16)
    return table.reshape(ROWS, times.shape[0])


def dot(a, b):
    return jnp.dot(a, b, preferred_element_type=F32)


def dot_t(a, b):
    return lax.dot_general(a, b, (((1,), (1,)), ((), ())), preferred_element_type=F32)


def same_freq(rows):
    row = lax.broadcasted_iota(jnp.int32, (rows, HALF), 0)
    col = lax.broadcasted_iota(jnp.int32, (rows, HALF), 1)
    return row % NF == col % NF


def pack_kernel(own, jobs, x_ref, *refs):
    outs, sems = refs[:-1], refs[-1]
    me = lax.axis_index("zh")
    copies = []
    for out, (shift, low) in zip(outs, jobs):
        side = (me + shift) % 2
        for d in range(out.shape[0]):
            start = ((d // 8) * 16 + d % 8) * own + low + side * (8 * own)
            cols = pl.ds(pl.multiple_of(start, 128), out.shape[2])
            copies.append(pltpu.make_async_copy(x_ref.at[:, cols], out.at[d], sems.at[len(copies)]))
    for copy in copies:
        copy.start()
    for copy in copies:
        copy.wait()


def pack(x, own, jobs):
    count = x.shape[1] // own // 2
    shapes = [jax.ShapeDtypeStruct((count, x.shape[0], n), x.dtype) for _, _, n in jobs]
    return pl.pallas_call(
        functools.partial(pack_kernel, own, [job[:2] for job in jobs]),
        out_shape=shapes,
        in_specs=[pl.BlockSpec(memory_space=pltpu.HBM)],
        out_specs=[pl.BlockSpec(memory_space=pltpu.VMEM)] * len(jobs),
        scratch_shapes=[pltpu.SemaphoreType.DMA((count * len(jobs),))],
        compiler_params=pltpu.CompilerParams(vmem_limit_bytes=60 * 2**20),
        name="pack",
    )(x)


def emit(parts, s_ref):
    for part in range(2):
        for b in range(NB):
            start = part * HALF + b * NF
            s_ref[b * 2 * NF + part * NF : b * 2 * NF + (part + 1) * NF, :] = parts[start : start + NF]


def gram_of(parts):
    real, imag = parts[:HALF], parts[HALF:]
    return jnp.concatenate([dot_t(real, real) + dot_t(imag, imag), dot_t(imag, real)], axis=0)


def rows_of(ref):
    return ref[...].reshape(-1, ref.shape[2])


def whole_kernel(w0_ref, w1_ref, x0_ref, x1_ref, s_ref, g_ref):
    parts = (dot(w0_ref[...], rows_of(x0_ref)) + dot(w1_ref[...], rows_of(x1_ref))).astype(BF16)
    emit(parts, s_ref)
    gram = gram_of(parts)

    @pl.when(pl.program_id(0) == 0)
    def _():
        g_ref[...] = gram

    @pl.when(pl.program_id(0) > 0)
    def _():
        g_ref[...] += gram


def whole(w0, w1, x0, x1, width):
    times = w0.shape[1]
    pts, count = x0.shape[2], x1.shape[2]
    skip = (pts - count) // width
    fixed = pl.BlockSpec((ROWS, times), lambda i: (0, 0))
    return pl.pallas_call(
        whole_kernel,
        grid=(count // width,),
        out_shape=(jax.ShapeDtypeStruct((ROWS, pts), BF16), jax.ShapeDtypeStruct((ROWS, HALF), F32)),
        in_specs=[
            fixed,
            fixed,
            pl.BlockSpec((*x0.shape[:2], width), lambda i: (0, 0, i + skip)),
            pl.BlockSpec((*x0.shape[:2], width), lambda i: (0, 0, i)),
        ],
        out_specs=(pl.BlockSpec((ROWS, width), lambda i: (0, i + skip)), pl.BlockSpec((ROWS, HALF), lambda i: (0, 0))),
        compiler_params=PARAMS,
        cost_estimate=pl.CostEstimate(flops=4 * ROWS * times * count, bytes_accessed=2**22, transcendentals=0),
        name="whole",
    )(w0, w1, x0, x1)


def partial_kernel(w_ref, x_ref, p_ref):
    p_ref[...] = dot(w_ref[...], rows_of(x_ref))


def partial(w, x, pts, width):
    times = w.shape[1]
    return pl.pallas_call(
        partial_kernel,
        grid=(pts // width,),
        out_shape=jax.ShapeDtypeStruct((ROWS, pts), F32),
        in_specs=[
            pl.BlockSpec((ROWS, times), lambda i: (0, 0)),
            pl.BlockSpec((*x.shape[:2], width), lambda i: (0, 0, i)),
        ],
        out_specs=pl.BlockSpec((ROWS, width), lambda i: (0, i)),
        compiler_params=PARAMS,
        cost_estimate=pl.CostEstimate(flops=2 * ROWS * times * pts, bytes_accessed=2**21, transcendentals=0),
        name="partial",
    )(w, x)


def lane_block(rows):
    return lax.broadcasted_iota(jnp.int32, (rows, HALF), 1) // NF


def turned(row, k):
    lane = lax.broadcasted_iota(jnp.int32, row.shape, 1)
    near = pltpu.roll(row, 256 - k * NF, 1)
    far = pltpu.roll(row, HALF - k * NF, 1)
    return jnp.where(lane < HALF - k * NF, near, far)


def rest_kernel(w_ref, x_ref, p_ref, g_ref, _, s_ref, t_ref, part_ref, row_ref, sem):
    width = x_ref.shape[2]
    parts = (p_ref[...] + dot(w_ref[...], rows_of(x_ref))).astype(BF16)
    emit(parts, part_ref)
    save = pltpu.make_async_copy(part_ref, s_ref.at[:, pl.ds(0, width)], sem)
    save.start()
    kept = jnp.where(same_freq(ROWS), g_ref[...] + gram_of(parts), 0.0)
    tables = kept.reshape(2 * NB, NF, HALF).sum(axis=1)
    block = lax.broadcasted_iota(jnp.int32, (NB, HALF), 0)
    row_ref[...] = jnp.zeros_like(row_ref)
    for k in range(NB):
        pick = (lane_block(NB) + k) % NB == block
        if k <= PAIRS:
            row_ref[k : k + 1, :HALF] = jnp.where(pick, tables[:NB], 0.0).sum(axis=0, keepdims=True)
        if k:
            row_ref[NB + k : NB + k + 1, :HALF] = jnp.where(pick, tables[NB:], 0.0).sum(axis=0, keepdims=True)
    rows = [row_ref[k : k + 1, :] for k in range(2 * NB)]
    imag = [rows[NB + k] - turned(rows[2 * NB - k], k) for k in range(1, PAIRS + 1)]
    sums = jnp.concatenate(rows[: PAIRS + 1] + imag + [jnp.zeros_like(imag[0])], axis=0)
    for i in range(t_ref.shape[0]):
        t_ref[i] = sums
    save.wait()


def rest(w, x, p, g, s, copies):
    times = w.shape[1]
    width = x.shape[2]
    here = pl.BlockSpec(memory_space=pltpu.VMEM)
    there = pl.BlockSpec(memory_space=pl.ANY)
    return pl.pallas_call(
        rest_kernel,
        out_shape=(jax.ShapeDtypeStruct(s.shape, BF16), jax.ShapeDtypeStruct((copies, 8, 256), F32)),
        in_specs=[here, here, here, here, there],
        out_specs=(there, here),
        scratch_shapes=[pltpu.VMEM((ROWS, width), BF16), pltpu.VMEM((16, 256), F32), pltpu.SemaphoreType.DMA],
        input_output_aliases={4: 0},
        compiler_params=pltpu.CompilerParams(vmem_limit_bytes=16 * 2**20),
        cost_estimate=pl.CostEstimate(flops=2 * ROWS * times * width, bytes_accessed=2**22, transcendentals=0),
        name="rest",
    )(w, x, p, g, s)


def spread_to(part):
    row = lax.broadcasted_iota(jnp.int32, (HALF, ROWS), 0)
    col = lax.broadcasted_iota(jnp.int32, (HALF, ROWS), 1)
    return (col == row // NF * 2 * NF + part * NF + row % NF).astype(BF16)


def power_kernel(denominator, t_ref, s_ref, o_ref, m_ref, in_ref, out_ref, in_sem, out_sem):
    steps, _, width = in_ref.shape
    loads = []
    for i in range(steps):
        loads.append(pltpu.make_async_copy(s_ref.at[:, pl.ds(i * width, width)], in_ref.at[i], in_sem.at[i]))
        loads[i].start()
    sums = jnp.sum(t_ref[...], axis=0) / denominator
    real_rows = [sums[k : k + 1, :] for k in range(PAIRS + 1)]
    imag_rows = [jnp.zeros_like(real_rows[0])] + [sums[PAIRS + k : PAIRS + k + 1, :] for k in range(1, PAIRS + 1)]
    for k in range(PAIRS + 1, NB):
        real_rows.append(turned(real_rows[NB - k], k))
        imag_rows.append(-turned(imag_rows[NB - k], k))
    block = lane_block(1)
    tables = []
    for rows in (real_rows, imag_rows):
        picked = [sum(jnp.where((block + k) % NB == b, rows[k][:, :HALF], 0.0) for k in range(NB)) for b in range(NB)]
        tables.append(jnp.concatenate(picked, axis=0).astype(BF16))
    real, imag = tables
    spread = [spread_to(part) for part in range(2)]
    from_real = dot(real, spread[0]) - dot(imag, spread[1])
    from_imag = dot(imag, spread[0]) + dot(real, spread[1])
    same = lax.broadcasted_iota(jnp.int32, (NF, ROWS), 0) == lax.broadcasted_iota(jnp.int32, (NF, ROWS), 1) % NF
    for b in range(NB):
        for part, table in enumerate((from_real, from_imag)):
            at = (2 * b + part) * NF
            row = jnp.broadcast_to(table[b : b + 1], (NF, ROWS))
            m_ref[at : at + NF, :] = jnp.where(same, row, 0.0).astype(BF16)
    stores = []
    for i in range(steps):
        loads[i].wait()
        out_ref[i] = dot(m_ref[...], in_ref[i])
        stores.append(pltpu.make_async_copy(out_ref.at[i], o_ref.at[:, pl.ds(i * width, width)], out_sem.at[i]))
        stores[i].start()
    for store in stores:
        store.wait()


def power(t, s, denominator):
    pts = s.shape[1]
    steps = pts // WIDTH
    return pl.pallas_call(
        functools.partial(power_kernel, denominator),
        out_shape=jax.ShapeDtypeStruct((ROWS, pts), F32),
        in_specs=[pl.BlockSpec(memory_space=pltpu.VMEM), pl.BlockSpec(memory_space=pl.ANY)],
        out_specs=pl.BlockSpec(memory_space=pl.ANY),
        scratch_shapes=[
            pltpu.VMEM((ROWS, ROWS), BF16),
            pltpu.VMEM((steps, ROWS, WIDTH), BF16),
            pltpu.VMEM((steps, ROWS, WIDTH), F32),
            pltpu.SemaphoreType.DMA((steps,)),
            pltpu.SemaphoreType.DMA((steps,)),
        ],
        compiler_params=pltpu.CompilerParams(vmem_limit_bytes=65_300_000),
        name="power",
    )(t, s)


def to_all(t, axes):
    copies = jnp.broadcast_to(t[None], (lax.axis_size(axes), *t.shape))
    return lax.all_to_all(copies, axes, 0, 0, tiled=True)


def exchange(x, axes):
    return lax.all_to_all(x, axes, 0, 0, tiled=True)


def shards(snapshots, block_starts, kept_freqs):
    count = lax.axis_size(TA)
    local = snapshots.shape[0]
    own = snapshots.shape[2] // count
    total = own * count * lax.axis_size("zl")
    swap = [(0, 1), (1, 0)]
    x = snapshots.reshape(local, own * count)

    later = own - FIRST
    (first,) = pack(x, own, [(1, later, FIRST)])
    first = lax.ppermute(first, "zh", swap)
    (pass_on,) = pack(x, own, [(1, 0, later)])
    pass_on = exchange(pass_on, PLANE)
    passed = lax.ppermute(pass_on, "zh", swap)
    (mine,) = pack(x, own, [(0, 0, own)])
    x0 = exchange(mine, PLANE)
    side = lax.axis_index("zh")
    place = jnp.arange(local * count // 2, dtype=jnp.int32)
    times = place // 128 * 256 + place % 128
    w0 = weights(block_starts, kept_freqs, times + side * 128)
    w1 = weights(block_starts, kept_freqs, times + (1 - side) * 128)
    first, w0, w1 = lax.optimization_barrier((first, w0, w1))
    first = exchange(first, PLANE)
    p = partial(w0, x0, later, 640)
    s, g = whole(w0, w1, x0, first, 256)
    s, t = rest(w1, passed, p, g, s, lax.axis_size(("y", "x")))
    t = exchange(t, ("y", "x")).sum(axis=0)
    t = to_all(t, ("zh", "zl", "c"))
    out = power(t, s, float(NB * total))
    shape = (1, NB, 2, NF, own)
    return s.reshape(shape), out.reshape(shape)


def solution(mesh):
    split = Mesh(mesh.devices.reshape(4, 2, 4, 2, mesh.shape["ga"]), ("y", "zh", "x", "c", "zl"))
    out = P("zl", None, None, None, TA)
    return jax.shard_map(
        shards, mesh=split, in_specs=(P(TA, "zl", None), P(), P()), out_specs=(out, out), check_vma=False
    )
```

```python
import functools
import math

import jax
import jax.numpy as jnp
from jax import lax
from jax.experimental import pallas as pl
from jax.experimental.pallas import tpu as pltpu
from jax.sharding import Mesh
from jax.sharding import PartitionSpec as P


NFFT = 256
NB = 7
NF = 32
HALF = NB * NF
ROWS = 2 * HALF
PAIRS = NB // 2
TA = ("y", "zh", "x", "c")
PLANE = ("y", "x", "c")
FIRST = 768
LAST = 512
F32 = jnp.float32
BF16 = jnp.bfloat16
SMALL = pltpu.CompilerParams(dimension_semantics=("arbitrary",), vmem_limit_bytes=16 * 2**20)
PARAMS = pltpu.CompilerParams(dimension_semantics=("arbitrary",), vmem_limit_bytes=60 * 2**20)


def weights(block_starts, kept_freqs, times):
    offset = times[None, :] - block_starts[:, None]
    inside = (offset >= 0) & (offset < NFFT)
    window = 0.5 - 0.5 * jnp.cos(2.0 * math.pi / NFFT * offset.astype(F32))
    scale = jnp.where(inside, window, 0.0)
    phase = kept_freqs[None, :, None] * jnp.where(inside, offset, 0)[:, None, :] % NFFT
    angle = 2.0 * math.pi / NFFT * phase.astype(F32)
    norm = 2.0 / math.sqrt(NFFT)
    real = scale[:, None, :] * jnp.cos(angle) * norm
    imag = -scale[:, None, :] * jnp.sin(angle) * norm
    table = jnp.stack([real, imag]).astype(BF16)
    return table.reshape(ROWS, times.shape[0])


def dot(a, b):
    return jnp.dot(a, b, preferred_element_type=F32)


def dot_t(a, b):
    return lax.dot_general(a, b, (((1,), (1,)), ((), ())), preferred_element_type=F32)


def same_freq(rows):
    row = lax.broadcasted_iota(jnp.int32, (rows, HALF), 0)
    col = lax.broadcasted_iota(jnp.int32, (rows, HALF), 1)
    return row % NF == col % NF


def pack_kernel(own, jobs, x_ref, *refs):
    outs, sems = refs[:-1], refs[-1]
    me = lax.axis_index("zh")
    copies = []
    for out, (shift, low) in zip(outs, jobs):
        side = (me + shift) % 2
        for d in range(out.shape[0]):
            start = ((d // 8) * 16 + d % 8) * own + low + side * (8 * own)
            cols = pl.ds(pl.multiple_of(start, 128), out.shape[2])
            copies.append(pltpu.make_async_copy(x_ref.at[:, cols], out.at[d], sems.at[len(copies)]))
    for copy in copies:
        copy.start()
    for copy in copies:
        copy.wait()


def pack(x, own, jobs):
    count = x.shape[1] // own // 2
    shapes = [jax.ShapeDtypeStruct((count, x.shape[0], n), x.dtype) for _, _, n in jobs]
    return pl.pallas_call(
        functools.partial(pack_kernel, own, [job[:2] for job in jobs]),
        out_shape=shapes,
        in_specs=[pl.BlockSpec(memory_space=pltpu.HBM)],
        out_specs=[pl.BlockSpec(memory_space=pltpu.VMEM)] * len(jobs),
        scratch_shapes=[pltpu.SemaphoreType.DMA((count * len(jobs),))],
        compiler_params=pltpu.CompilerParams(vmem_limit_bytes=60 * 2**20),
        name="pack",
    )(x)


def emit(parts, s_ref):
    for part in range(2):
        for b in range(NB):
            start = part * HALF + b * NF
            s_ref[b * 2 * NF + part * NF : b * 2 * NF + (part + 1) * NF, :] = parts[start : start + NF]


def gram_of(parts):
    real, imag = parts[:HALF], parts[HALF:]
    return jnp.concatenate([dot_t(real, real) + dot_t(imag, imag), dot_t(imag, real)], axis=0)


def rows_of(ref):
    return ref[...].reshape(-1, ref.shape[2])


def whole_kernel(w0_ref, w1_ref, x0_ref, x1_ref, s_ref, g_ref, part_ref):
    parts = (dot(w0_ref[...], rows_of(x0_ref)) + dot(w1_ref[...], rows_of(x1_ref))).astype(BF16)
    emit(parts, s_ref)
    emit(parts, part_ref)
    gram = gram_of(parts)

    @pl.when(pl.program_id(0) == 0)
    def _():
        g_ref[...] = gram

    @pl.when(pl.program_id(0) > 0)
    def _():
        g_ref[...] += gram


def whole(w0, w1, x0, x1, width):
    times = w0.shape[1]
    pts, count = x0.shape[2], x1.shape[2]
    skip = (pts - count) // width
    fixed = pl.BlockSpec((ROWS, times), lambda i: (0, 0))
    return pl.pallas_call(
        whole_kernel,
        grid=(count // width,),
        out_shape=(
            jax.ShapeDtypeStruct((ROWS, pts), BF16),
            jax.ShapeDtypeStruct((ROWS, HALF), F32),
            jax.ShapeDtypeStruct((ROWS, count), BF16),
        ),
        in_specs=[
            fixed,
            fixed,
            pl.BlockSpec((*x0.shape[:2], width), lambda i: (0, 0, i + skip)),
            pl.BlockSpec((*x0.shape[:2], width), lambda i: (0, 0, i)),
        ],
        out_specs=(
            pl.BlockSpec((ROWS, width), lambda i: (0, i + skip)),
            pl.BlockSpec((ROWS, HALF), lambda i: (0, 0)),
            pl.BlockSpec((ROWS, width), lambda i: (0, i)),
        ),
        compiler_params=SMALL,
        cost_estimate=pl.CostEstimate(flops=4 * ROWS * times * count, bytes_accessed=2**22, transcendentals=0),
        name="whole",
    )(w0, w1, x0, x1)


def partial_kernel(w_ref, x_ref, p_ref):
    p_ref[...] = dot(w_ref[...], rows_of(x_ref))


def partial(w, x, low, pts, width):
    times = w.shape[1]
    skip = low // width
    return pl.pallas_call(
        partial_kernel,
        grid=(pts // width,),
        out_shape=jax.ShapeDtypeStruct((ROWS, pts), F32),
        in_specs=[
            pl.BlockSpec((ROWS, times), lambda i: (0, 0)),
            pl.BlockSpec((*x.shape[:2], width), lambda i: (0, 0, i + skip)),
        ],
        out_specs=pl.BlockSpec((ROWS, width), lambda i: (0, i)),
        compiler_params=PARAMS,
        cost_estimate=pl.CostEstimate(flops=2 * ROWS * times * pts, bytes_accessed=2**21, transcendentals=0),
        name="partial",
    )(w, x)


def lane_block(rows):
    return lax.broadcasted_iota(jnp.int32, (rows, HALF), 1) // NF


def turned(row, k):
    lane = lax.broadcasted_iota(jnp.int32, row.shape, 1)
    near = pltpu.roll(row, 256 - k * NF, 1)
    far = pltpu.roll(row, HALF - k * NF, 1)
    return jnp.where(lane < HALF - k * NF, near, far)


def middle_kernel(w_ref, x_ref, p_ref, g_ref, _, s_ref, out_ref, part_ref):
    parts = (p_ref[...] + dot(w_ref[...], rows_of(x_ref))).astype(BF16)
    emit(parts, s_ref)
    emit(parts, part_ref)
    out_ref[...] = g_ref[...] + gram_of(parts)


def middle(w, x, p, g, s):
    times = w.shape[1]
    width = x.shape[2]
    here = pl.BlockSpec(memory_space=pltpu.VMEM)
    return pl.pallas_call(
        middle_kernel,
        grid=(1,),
        out_shape=(
            jax.ShapeDtypeStruct(s.shape, BF16),
            jax.ShapeDtypeStruct((ROWS, HALF), F32),
            jax.ShapeDtypeStruct((ROWS, width), BF16),
        ),
        in_specs=[here, here, here, here, pl.BlockSpec(memory_space=pl.ANY)],
        out_specs=(pl.BlockSpec((ROWS, width), lambda i: (0, 0)), here, here),
        input_output_aliases={4: 0},
        compiler_params=SMALL,
        cost_estimate=pl.CostEstimate(flops=2 * ROWS * times * width, bytes_accessed=2**22, transcendentals=0),
        name="middle",
    )(w, x, p, g, s)


def rest_kernel(low, w_ref, x_ref, p_ref, g_ref, _, s_ref, t_ref, part_ref, row_ref, sem):
    width = x_ref.shape[2]
    parts = (p_ref[...] + dot(w_ref[...], rows_of(x_ref))).astype(BF16)
    emit(parts, part_ref)
    save = pltpu.make_async_copy(part_ref, s_ref.at[:, pl.ds(low, width)], sem)
    save.start()
    kept = jnp.where(same_freq(ROWS), g_ref[...] + gram_of(parts), 0.0)
    tables = kept.reshape(2 * NB, NF, HALF).sum(axis=1)
    block = lax.broadcasted_iota(jnp.int32, (NB, HALF), 0)
    row_ref[...] = jnp.zeros_like(row_ref)
    for k in range(NB):
        pick = (lane_block(NB) + k) % NB == block
        if k <= PAIRS:
            row_ref[k : k + 1, :HALF] = jnp.where(pick, tables[:NB], 0.0).sum(axis=0, keepdims=True)
        if k:
            row_ref[NB + k : NB + k + 1, :HALF] = jnp.where(pick, tables[NB:], 0.0).sum(axis=0, keepdims=True)
    rows = [row_ref[k : k + 1, :] for k in range(2 * NB)]
    imag = [rows[NB + k] - turned(rows[2 * NB - k], k) for k in range(1, PAIRS + 1)]
    sums = jnp.concatenate(rows[: PAIRS + 1] + imag + [jnp.zeros_like(imag[0])], axis=0)
    for i in range(t_ref.shape[0]):
        t_ref[i] = sums
    save.wait()


def rest(w, x, p, g, s, low, copies):
    times = w.shape[1]
    width = x.shape[2]
    here = pl.BlockSpec(memory_space=pltpu.VMEM)
    there = pl.BlockSpec(memory_space=pl.ANY)
    return pl.pallas_call(
        functools.partial(rest_kernel, low),
        out_shape=(
            jax.ShapeDtypeStruct(s.shape, BF16),
            jax.ShapeDtypeStruct((copies, 8, 256), F32),
            jax.ShapeDtypeStruct((ROWS, width), BF16),
        ),
        in_specs=[here, here, here, here, there],
        out_specs=(there, here, here),
        scratch_shapes=[pltpu.VMEM((16, 256), F32), pltpu.SemaphoreType.DMA],
        input_output_aliases={4: 0},
        compiler_params=pltpu.CompilerParams(vmem_limit_bytes=16 * 2**20),
        cost_estimate=pl.CostEstimate(flops=2 * ROWS * times * width, bytes_accessed=2**22, transcendentals=0),
        name="rest",
    )(w, x, p, g, s)


def spread_to(part):
    row = lax.broadcasted_iota(jnp.int32, (HALF, ROWS), 0)
    col = lax.broadcasted_iota(jnp.int32, (HALF, ROWS), 1)
    return (col == row // NF * 2 * NF + part * NF + row % NF).astype(BF16)


def power_kernel(denominator, t_ref, *refs):
    part_refs, (o_ref, m_ref, out_ref, sem) = refs[:-4], refs[-4:]
    sums = jnp.sum(t_ref[...], axis=0) / denominator
    real_rows = [sums[k : k + 1, :] for k in range(PAIRS + 1)]
    imag_rows = [jnp.zeros_like(real_rows[0])] + [sums[PAIRS + k : PAIRS + k + 1, :] for k in range(1, PAIRS + 1)]
    for k in range(PAIRS + 1, NB):
        real_rows.append(turned(real_rows[NB - k], k))
        imag_rows.append(-turned(imag_rows[NB - k], k))
    block = lane_block(1)
    tables = []
    for rows in (real_rows, imag_rows):
        picked = [sum(jnp.where((block + k) % NB == b, rows[k][:, :HALF], 0.0) for k in range(NB)) for b in range(NB)]
        tables.append(jnp.concatenate(picked, axis=0).astype(BF16))
    real, imag = tables
    spread = [spread_to(part) for part in range(2)]
    from_real = dot(real, spread[0]) - dot(imag, spread[1])
    from_imag = dot(imag, spread[0]) + dot(real, spread[1])
    same = lax.broadcasted_iota(jnp.int32, (NF, ROWS), 0) == lax.broadcasted_iota(jnp.int32, (NF, ROWS), 1) % NF
    for b in range(NB):
        for part, table in enumerate((from_real, from_imag)):
            at = (2 * b + part) * NF
            row = jnp.broadcast_to(table[b : b + 1], (NF, ROWS))
            m_ref[at : at + NF, :] = jnp.where(same, row, 0.0).astype(BF16)
    stores = []
    low = 0
    for part_ref in part_refs:
        for at in range(0, part_ref.shape[1], 512):
            values = part_ref[:, at : at + 512]
            cols = pl.ds(low, values.shape[1])
            out_ref[:, low : low + values.shape[1]] = dot(m_ref[...], values)
            stores.append(pltpu.make_async_copy(out_ref.at[:, cols], o_ref.at[:, cols], sem.at[len(stores)]))
            stores[-1].start()
            low += values.shape[1]
    for store in stores:
        store.wait()


def power(t, parts, denominator):
    pts = sum(part.shape[1] for part in parts)
    here = pl.BlockSpec(memory_space=pltpu.VMEM)
    return pl.pallas_call(
        functools.partial(power_kernel, denominator),
        out_shape=jax.ShapeDtypeStruct((ROWS, pts), F32),
        in_specs=[here] * (1 + len(parts)),
        out_specs=pl.BlockSpec(memory_space=pl.ANY),
        scratch_shapes=[
            pltpu.VMEM((ROWS, ROWS), BF16),
            pltpu.VMEM((ROWS, pts), F32),
            pltpu.SemaphoreType.DMA((8,)),
        ],
        compiler_params=pltpu.CompilerParams(vmem_limit_bytes=16 * 2**20),
        name="power",
    )(t, *parts)


def to_all(t, axes):
    copies = jnp.broadcast_to(t[None], (lax.axis_size(axes), *t.shape))
    return lax.all_to_all(copies, axes, 0, 0, tiled=True)


def exchange(x, axes):
    return lax.all_to_all(x, axes, 0, 0, tiled=True)


def shards(snapshots, block_starts, kept_freqs):
    count = lax.axis_size(TA)
    local = snapshots.shape[0]
    own = snapshots.shape[2] // count
    total = own * count * lax.axis_size("zl")
    swap = [(0, 1), (1, 0)]
    x = snapshots.reshape(local, own * count)

    later = own - FIRST
    low = later - LAST
    (first,) = pack(x, own, [(1, later, FIRST)])
    first = lax.ppermute(first, "zh", swap)
    (pass_on,) = pack(x, own, [(1, 0, later)])
    pass_on = exchange(pass_on, PLANE)
    passed = lax.ppermute(pass_on[:, :, :low], "zh", swap)
    last = lax.ppermute(pass_on[:, :, low:], "zh", swap)
    (mine,) = pack(x, own, [(0, 0, own)])
    x0 = exchange(mine, PLANE)
    side = lax.axis_index("zh")
    place = jnp.arange(local * count // 2, dtype=jnp.int32)
    times = place // 128 * 256 + place % 128
    w0 = weights(block_starts, kept_freqs, times + side * 128)
    w1 = weights(block_starts, kept_freqs, times + (1 - side) * 128)
    first, w0, w1 = lax.optimization_barrier((first, w0, w1))
    first = exchange(first, PLANE)
    p0 = partial(w0, x0, 0, low, 256)
    p1 = partial(w0, x0, low, LAST, 256)
    s, g, part2 = whole(w0, w1, x0, first, 256)
    s, g, part0 = middle(w1, passed, p0, g, s)
    s, t, part1 = rest(w1, last, p1, g, s, low, lax.axis_size(("y", "x")))
    t = exchange(t, ("y", "x")).sum(axis=0)
    t = to_all(t, ("zh", "zl", "c"))
    out = power(t, (part0, part1, part2), float(NB * total))
    shape = (1, NB, 2, NF, own)
    return s.reshape(shape), out.reshape(shape)


def solution(mesh):
    split = Mesh(mesh.devices.reshape(4, 2, 4, 2, mesh.shape["ga"]), ("y", "zh", "x", "c", "zl"))
    out = P("zl", None, None, None, TA)
    return jax.shard_map(
        shards, mesh=split, in_specs=(P(TA, "zl", None), P(), P()), out_specs=(out, out), check_vma=False
    )
```

```python
import functools
import math

import jax
import jax.numpy as jnp
from jax import lax
from jax.experimental import pallas as pl
from jax.experimental.pallas import tpu as pltpu
from jax.sharding import Mesh
from jax.sharding import PartitionSpec as P


NFFT = 256
NB = 7
NF = 32
HALF = NB * NF
ROWS = 2 * HALF
PAIRS = NB // 2
TA = ("y", "zh", "x", "c")
PLANE = ("y", "x", "c")
FIRST = 640
LAST = 512
F32 = jnp.float32
BF16 = jnp.bfloat16


def weights(block_starts, kept_freqs, times):
    offset = times[None, :] - block_starts[:, None]
    inside = (offset >= 0) & (offset < NFFT)
    window = 0.5 - 0.5 * jnp.cos(2.0 * math.pi / NFFT * offset.astype(F32))
    scale = jnp.where(inside, window, 0.0)
    phase = kept_freqs[None, :, None] * jnp.where(inside, offset, 0)[:, None, :] % NFFT
    angle = 2.0 * math.pi / NFFT * phase.astype(F32)
    norm = 2.0 / math.sqrt(NFFT)
    real = scale[:, None, :] * jnp.cos(angle) * norm
    imag = -scale[:, None, :] * jnp.sin(angle) * norm
    table = jnp.stack([real, imag]).astype(BF16)
    return table.reshape(ROWS, times.shape[0])


def dot(a, b):
    return jnp.dot(a, b, preferred_element_type=F32)


def dot_t(a, b):
    return lax.dot_general(a, b, (((1,), (1,)), ((), ())), preferred_element_type=F32)


def same_freq(rows):
    row = lax.broadcasted_iota(jnp.int32, (rows, HALF), 0)
    col = lax.broadcasted_iota(jnp.int32, (rows, HALF), 1)
    return row % NF == col % NF


def pack_kernel(own, jobs, x_ref, *refs):
    outs, sems = refs[:-1], refs[-1]
    me = lax.axis_index("zh")
    copies = []
    for out, (shift, low) in zip(outs, jobs):
        side = (me + shift) % 2
        for d in range(out.shape[0]):
            start = ((d // 8) * 16 + d % 8) * own + low + side * (8 * own)
            cols = pl.ds(pl.multiple_of(start, 128), out.shape[2])
            copies.append(pltpu.make_async_copy(x_ref.at[:, cols], out.at[d], sems.at[len(copies)]))
    for copy in copies:
        copy.start()
    for copy in copies:
        copy.wait()


def pack(x, own, jobs):
    count = x.shape[1] // own // 2
    shapes = [jax.ShapeDtypeStruct((count, x.shape[0], n), x.dtype) for _, _, n in jobs]
    return pl.pallas_call(
        functools.partial(pack_kernel, own, [job[:2] for job in jobs]),
        out_shape=shapes,
        in_specs=[pl.BlockSpec(memory_space=pltpu.HBM)],
        out_specs=[pl.BlockSpec(memory_space=pltpu.VMEM)] * len(jobs),
        scratch_shapes=[pltpu.SemaphoreType.DMA((count * len(jobs),))],
        compiler_params=pltpu.CompilerParams(vmem_limit_bytes=60 * 2**20),
        name="pack",
    )(x)


def emit(parts, s_ref):
    for part in range(2):
        for b in range(NB):
            start = part * HALF + b * NF
            s_ref[b * 2 * NF + part * NF : b * 2 * NF + (part + 1) * NF, :] = parts[start : start + NF]


def gram_of(parts):
    real, imag = parts[:HALF], parts[HALF:]
    return jnp.concatenate([dot_t(real, real) + dot_t(imag, imag), dot_t(imag, real)], axis=0)


def rows_of(ref):
    return ref[...].reshape(-1, ref.shape[2])


def whole_kernel(w0_ref, w1_ref, x0_ref, x1_ref, g_ref, _, s_ref, out_ref, part_ref, sem):
    count = x1_ref.shape[2]
    low = x0_ref.shape[2] - count
    near = x0_ref[:, :, low:].reshape(-1, count)
    parts = (dot(w0_ref[...], near) + dot(w1_ref[...], rows_of(x1_ref))).astype(BF16)
    emit(parts, part_ref)
    save = pltpu.make_async_copy(part_ref, s_ref.at[:, pl.ds(low, count)], sem)
    save.start()
    out_ref[...] = g_ref[...] + gram_of(parts)
    save.wait()


def whole(w0, w1, x0, x1, g, s):
    times = w0.shape[1]
    count = x1.shape[2]
    here = pl.BlockSpec(memory_space=pltpu.VMEM)
    there = pl.BlockSpec(memory_space=pl.ANY)
    return pl.pallas_call(
        whole_kernel,
        out_shape=(
            jax.ShapeDtypeStruct(s.shape, BF16),
            jax.ShapeDtypeStruct((ROWS, HALF), F32),
            jax.ShapeDtypeStruct((ROWS, count), BF16),
        ),
        in_specs=[here] * 5 + [there],
        out_specs=(there, here, here),
        scratch_shapes=[pltpu.SemaphoreType.DMA],
        input_output_aliases={5: 0},
        compiler_params=pltpu.CompilerParams(vmem_limit_bytes=16 * 2**20),
        cost_estimate=pl.CostEstimate(flops=4 * ROWS * times * count, bytes_accessed=2**22, transcendentals=0),
        name="whole",
    )(w0, w1, x0, x1, g, s)


def partial_kernel(w_ref, x_ref, *p_refs):
    low = 0
    for p_ref in p_refs:
        count = p_ref.shape[1]
        p_ref[...] = dot(w_ref[...], x_ref[:, :, low : low + count].reshape(-1, count))
        low += count


def partial(w, x, counts):
    times = w.shape[1]
    here = pl.BlockSpec(memory_space=pltpu.VMEM)
    return pl.pallas_call(
        partial_kernel,
        out_shape=[jax.ShapeDtypeStruct((ROWS, count), F32) for count in counts],
        in_specs=[here, here],
        out_specs=[here] * len(counts),
        compiler_params=pltpu.CompilerParams(vmem_limit_bytes=16 * 2**20),
        cost_estimate=pl.CostEstimate(flops=2 * ROWS * times * sum(counts), bytes_accessed=2**21, transcendentals=0),
        name="partial",
    )(w, x)


def lane_block(rows):
    return lax.broadcasted_iota(jnp.int32, (rows, HALF), 1) // NF


def turned(row, k):
    lane = lax.broadcasted_iota(jnp.int32, row.shape, 1)
    near = pltpu.roll(row, 256 - k * NF, 1)
    far = pltpu.roll(row, HALF - k * NF, 1)
    return jnp.where(lane < HALF - k * NF, near, far)


def middle_kernel(w_ref, x_ref, p_ref, s_ref, out_ref, part_ref, sem):
    parts = (p_ref[...] + dot(w_ref[...], rows_of(x_ref))).astype(BF16)
    emit(parts, part_ref)
    save = pltpu.make_async_copy(part_ref, s_ref.at[:, pl.ds(0, parts.shape[1])], sem)
    save.start()
    out_ref[...] = gram_of(parts)
    save.wait()


def middle(w, x, p, pts):
    times = w.shape[1]
    width = x.shape[2]
    here = pl.BlockSpec(memory_space=pltpu.VMEM)
    return pl.pallas_call(
        middle_kernel,
        out_shape=(
            jax.ShapeDtypeStruct((ROWS, pts), BF16),
            jax.ShapeDtypeStruct((ROWS, HALF), F32),
            jax.ShapeDtypeStruct((ROWS, width), BF16),
        ),
        in_specs=[here] * 3,
        out_specs=(pl.BlockSpec(memory_space=pl.ANY), here, here),
        scratch_shapes=[pltpu.SemaphoreType.DMA],
        compiler_params=pltpu.CompilerParams(vmem_limit_bytes=16 * 2**20),
        cost_estimate=pl.CostEstimate(flops=2 * ROWS * times * width, bytes_accessed=2**22, transcendentals=0),
        name="middle",
    )(w, x, p)


def rest_kernel(low, w_ref, x_ref, p_ref, g_ref, _, s_ref, t_ref, part_ref, row_ref, sem):
    width = x_ref.shape[2]
    parts = (p_ref[...] + dot(w_ref[...], rows_of(x_ref))).astype(BF16)
    emit(parts, part_ref)
    save = pltpu.make_async_copy(part_ref, s_ref.at[:, pl.ds(low, width)], sem)
    save.start()
    kept = jnp.where(same_freq(ROWS), g_ref[...] + gram_of(parts), 0.0)
    tables = kept.reshape(2 * NB, NF, HALF).sum(axis=1)
    block = lax.broadcasted_iota(jnp.int32, (NB, HALF), 0)
    row_ref[...] = jnp.zeros_like(row_ref)
    for k in range(NB):
        pick = (lane_block(NB) + k) % NB == block
        if k <= PAIRS:
            row_ref[k : k + 1, :HALF] = jnp.where(pick, tables[:NB], 0.0).sum(axis=0, keepdims=True)
        if k:
            row_ref[NB + k : NB + k + 1, :HALF] = jnp.where(pick, tables[NB:], 0.0).sum(axis=0, keepdims=True)
    rows = [row_ref[k : k + 1, :] for k in range(2 * NB)]
    imag = [rows[NB + k] - turned(rows[2 * NB - k], k) for k in range(1, PAIRS + 1)]
    sums = jnp.concatenate(rows[: PAIRS + 1] + imag + [jnp.zeros_like(imag[0])], axis=0)
    for i in range(t_ref.shape[0]):
        t_ref[i] = sums
    save.wait()


def rest(w, x, p, g, s, low, copies):
    times = w.shape[1]
    width = x.shape[2]
    here = pl.BlockSpec(memory_space=pltpu.VMEM)
    there = pl.BlockSpec(memory_space=pl.ANY)
    return pl.pallas_call(
        functools.partial(rest_kernel, low),
        out_shape=(
            jax.ShapeDtypeStruct(s.shape, BF16),
            jax.ShapeDtypeStruct((copies, 8, 256), F32),
            jax.ShapeDtypeStruct((ROWS, width), BF16),
        ),
        in_specs=[here, here, here, here, there],
        out_specs=(there, here, here),
        scratch_shapes=[pltpu.VMEM((16, 256), F32), pltpu.SemaphoreType.DMA],
        input_output_aliases={4: 0},
        compiler_params=pltpu.CompilerParams(vmem_limit_bytes=16 * 2**20),
        cost_estimate=pl.CostEstimate(flops=2 * ROWS * times * width, bytes_accessed=2**22, transcendentals=0),
        name="rest",
    )(w, x, p, g, s)


def spread_to(part):
    row = lax.broadcasted_iota(jnp.int32, (HALF, ROWS), 0)
    col = lax.broadcasted_iota(jnp.int32, (HALF, ROWS), 1)
    return (col == row // NF * 2 * NF + part * NF + row % NF).astype(BF16)


def power_kernel(denominator, t_ref, *refs):
    part_refs, (o_ref, m_ref, out_ref, sem) = refs[:-4], refs[-4:]
    sums = jnp.sum(t_ref[...], axis=0) / denominator
    real_rows = [sums[k : k + 1, :] for k in range(PAIRS + 1)]
    imag_rows = [jnp.zeros_like(real_rows[0])] + [sums[PAIRS + k : PAIRS + k + 1, :] for k in range(1, PAIRS + 1)]
    for k in range(PAIRS + 1, NB):
        real_rows.append(turned(real_rows[NB - k], k))
        imag_rows.append(-turned(imag_rows[NB - k], k))
    block = lane_block(1)
    tables = []
    for rows in (real_rows, imag_rows):
        picked = [sum(jnp.where((block + k) % NB == b, rows[k][:, :HALF], 0.0) for k in range(NB)) for b in range(NB)]
        tables.append(jnp.concatenate(picked, axis=0).astype(BF16))
    real, imag = tables
    spread = [spread_to(part) for part in range(2)]
    from_real = dot(real, spread[0]) - dot(imag, spread[1])
    from_imag = dot(imag, spread[0]) + dot(real, spread[1])
    same = lax.broadcasted_iota(jnp.int32, (NF, ROWS), 0) == lax.broadcasted_iota(jnp.int32, (NF, ROWS), 1) % NF
    for b in range(NB):
        for part, table in enumerate((from_real, from_imag)):
            at = (2 * b + part) * NF
            row = jnp.broadcast_to(table[b : b + 1], (NF, ROWS))
            m_ref[at : at + NF, :] = jnp.where(same, row, 0.0).astype(BF16)
    stores = []
    low = 0
    for part_ref in part_refs:
        for at in range(0, part_ref.shape[1], 512):
            values = part_ref[:, at : at + 512]
            cols = pl.ds(low, values.shape[1])
            out_ref[:, low : low + values.shape[1]] = dot(m_ref[...], values)
            stores.append(pltpu.make_async_copy(out_ref.at[:, cols], o_ref.at[:, cols], sem.at[len(stores)]))
            stores[-1].start()
            low += values.shape[1]
    for store in stores:
        store.wait()


def power(t, parts, denominator):
    pts = sum(part.shape[1] for part in parts)
    here = pl.BlockSpec(memory_space=pltpu.VMEM)
    return pl.pallas_call(
        functools.partial(power_kernel, denominator),
        out_shape=jax.ShapeDtypeStruct((ROWS, pts), F32),
        in_specs=[here] * (1 + len(parts)),
        out_specs=pl.BlockSpec(memory_space=pl.ANY),
        scratch_shapes=[
            pltpu.VMEM((ROWS, ROWS), BF16),
            pltpu.VMEM((ROWS, pts), F32),
            pltpu.SemaphoreType.DMA((8,)),
        ],
        compiler_params=pltpu.CompilerParams(vmem_limit_bytes=16 * 2**20),
        name="power",
    )(t, *parts)


def to_all(t, axes):
    copies = jnp.broadcast_to(t[None], (lax.axis_size(axes), *t.shape))
    return lax.all_to_all(copies, axes, 0, 0, tiled=True)


def exchange(x, axes):
    return lax.all_to_all(x, axes, 0, 0, tiled=True)


def shards(snapshots, block_starts, kept_freqs):
    count = lax.axis_size(TA)
    local = snapshots.shape[0]
    own = snapshots.shape[2] // count
    total = own * count * lax.axis_size("zl")
    swap = [(0, 1), (1, 0)]
    x = snapshots.reshape(local, own * count)

    later = own - FIRST
    low = later - LAST
    (first,) = pack(x, own, [(1, later, FIRST)])
    first = lax.ppermute(first, "zh", swap)
    (pass_on,) = pack(x, own, [(1, 0, later)])
    pass_on = exchange(pass_on, PLANE)
    passed = lax.ppermute(pass_on[:, :, :low], "zh", swap)
    last = lax.ppermute(pass_on[:, :, low:], "zh", swap)
    (mine,) = pack(x, own, [(0, 0, own)])
    x0 = exchange(mine, PLANE)
    side = lax.axis_index("zh")
    place = jnp.arange(local * count // 2, dtype=jnp.int32)
    times = place // 128 * 256 + place % 128
    w0 = weights(block_starts, kept_freqs, times + side * 128)
    w1 = weights(block_starts, kept_freqs, times + (1 - side) * 128)
    first, w0, w1 = lax.optimization_barrier((first, w0, w1))
    first = exchange(first, PLANE)
    p0, p1 = partial(w0, x0, (low, LAST))
    s, g, part0 = middle(w1, passed, p0, own)
    s, g, part2 = whole(w0, w1, x0, first, g, s)
    s, t, part1 = rest(w1, last, p1, g, s, low, lax.axis_size(("y", "x")))
    t = exchange(t, ("y", "x")).sum(axis=0)
    t = to_all(t, ("zh", "zl", "c"))
    out = power(t, (part0, part1, part2), float(NB * total))
    shape = (1, NB, 2, NF, own)
    return s.reshape(shape), out.reshape(shape)


def solution(mesh):
    split = Mesh(mesh.devices.reshape(4, 2, 4, 2, mesh.shape["ga"]), ("y", "zh", "x", "c", "zl"))
    out = P("zl", None, None, None, TA)
    return jax.shard_map(
        shards, mesh=split, in_specs=(P(TA, "zl", None), P(), P()), out_specs=(out, out), check_vma=False
    )
```

```python
import functools
import math

import jax
import jax.numpy as jnp
from jax import lax
from jax.experimental import pallas as pl
from jax.experimental.pallas import tpu as pltpu
from jax.sharding import Mesh
from jax.sharding import PartitionSpec as P


NFFT = 256
NB = 7
NF = 32
HALF = NB * NF
ROWS = 2 * HALF
PAIRS = NB // 2
TA = ("y", "zh", "x", "c")
PLANE = ("y", "x", "c")
FIRST = 768
LAST = 512
F32 = jnp.float32
BF16 = jnp.bfloat16


def weights(block_starts, kept_freqs, times):
    offset = times[None, :] - block_starts[:, None]
    inside = (offset >= 0) & (offset < NFFT)
    window = 0.5 - 0.5 * jnp.cos(2.0 * math.pi / NFFT * offset.astype(F32))
    scale = jnp.where(inside, window, 0.0)
    phase = kept_freqs[None, :, None] * jnp.where(inside, offset, 0)[:, None, :] % NFFT
    angle = 2.0 * math.pi / NFFT * phase.astype(F32)
    norm = 2.0 / math.sqrt(NFFT)
    real = scale[:, None, :] * jnp.cos(angle) * norm
    imag = -scale[:, None, :] * jnp.sin(angle) * norm
    table = jnp.stack([real, imag]).astype(BF16)
    return table.reshape(ROWS, times.shape[0])


def dot(a, b):
    return jnp.dot(a, b, preferred_element_type=F32)


def dot_t(a, b):
    return lax.dot_general(a, b, (((1,), (1,)), ((), ())), preferred_element_type=F32)


def same_freq(rows):
    row = lax.broadcasted_iota(jnp.int32, (rows, HALF), 0)
    col = lax.broadcasted_iota(jnp.int32, (rows, HALF), 1)
    return row % NF == col % NF


def pack_kernel(own, jobs, x_ref, *refs):
    outs, sems = refs[:-1], refs[-1]
    me = lax.axis_index("zh")
    copies = []
    for out, (shift, low) in zip(outs, jobs):
        side = (me + shift) % 2
        for d in range(out.shape[0]):
            start = ((d // 8) * 16 + d % 8) * own + low + side * (8 * own)
            cols = pl.ds(pl.multiple_of(start, 128), out.shape[2])
            copies.append(pltpu.make_async_copy(x_ref.at[:, cols], out.at[d], sems.at[len(copies)]))
    for copy in copies:
        copy.start()
    for copy in copies:
        copy.wait()


def pack(x, own, jobs):
    count = x.shape[1] // own // 2
    shapes = [jax.ShapeDtypeStruct((count, x.shape[0], n), x.dtype) for _, _, n in jobs]
    return pl.pallas_call(
        functools.partial(pack_kernel, own, [job[:2] for job in jobs]),
        out_shape=shapes,
        in_specs=[pl.BlockSpec(memory_space=pltpu.HBM)],
        out_specs=[pl.BlockSpec(memory_space=pltpu.VMEM)] * len(jobs),
        scratch_shapes=[pltpu.SemaphoreType.DMA((count * len(jobs),))],
        compiler_params=pltpu.CompilerParams(vmem_limit_bytes=60 * 2**20),
        name="pack",
    )(x)


def emit(parts, s_ref):
    for part in range(2):
        for b in range(NB):
            start = part * HALF + b * NF
            s_ref[b * 2 * NF + part * NF : b * 2 * NF + (part + 1) * NF, :] = parts[start : start + NF]


def gram_of(parts):
    real, imag = parts[:HALF], parts[HALF:]
    return jnp.concatenate([dot_t(real, real) + dot_t(imag, imag), dot_t(imag, real)], axis=0)


def rows_of(ref):
    return ref[...].reshape(-1, ref.shape[2])


def whole_kernel(w0_ref, w1_ref, x0_ref, x1_ref, _, s_ref, out_ref, part_ref, sem):
    count = x1_ref.shape[2]
    low = x0_ref.shape[2] - count
    near = x0_ref[:, :, low:].reshape(-1, count)
    parts = (dot(w0_ref[...], near) + dot(w1_ref[...], rows_of(x1_ref))).astype(BF16)
    emit(parts, part_ref)
    save = pltpu.make_async_copy(part_ref, s_ref.at[:, pl.ds(low, count)], sem)
    save.start()
    out_ref[...] = gram_of(parts)
    save.wait()


def whole(w0, w1, x0, x1, s):
    times = w0.shape[1]
    count = x1.shape[2]
    here = pl.BlockSpec(memory_space=pltpu.VMEM)
    there = pl.BlockSpec(memory_space=pl.ANY)
    return pl.pallas_call(
        whole_kernel,
        out_shape=(
            jax.ShapeDtypeStruct(s.shape, BF16),
            jax.ShapeDtypeStruct((ROWS, HALF), F32),
            jax.ShapeDtypeStruct((ROWS, count), BF16),
        ),
        in_specs=[here] * 4 + [there],
        out_specs=(there, here, here),
        scratch_shapes=[pltpu.SemaphoreType.DMA],
        input_output_aliases={4: 0},
        compiler_params=pltpu.CompilerParams(vmem_limit_bytes=16 * 2**20),
        cost_estimate=pl.CostEstimate(flops=4 * ROWS * times * count, bytes_accessed=2**22, transcendentals=0),
        name="whole",
    )(w0, w1, x0, x1, s)


def partial_kernel(w_ref, x_ref, *p_refs):
    low = 0
    for p_ref in p_refs:
        count = p_ref.shape[1]
        p_ref[...] = dot(w_ref[...], x_ref[:, :, low : low + count].reshape(-1, count))
        low += count


def partial(w, x, counts):
    times = w.shape[1]
    here = pl.BlockSpec(memory_space=pltpu.VMEM)
    return pl.pallas_call(
        partial_kernel,
        out_shape=[jax.ShapeDtypeStruct((ROWS, count), F32) for count in counts],
        in_specs=[here, here],
        out_specs=[here] * len(counts),
        compiler_params=pltpu.CompilerParams(vmem_limit_bytes=16 * 2**20),
        cost_estimate=pl.CostEstimate(flops=2 * ROWS * times * sum(counts), bytes_accessed=2**21, transcendentals=0),
        name="partial",
    )(w, x)


def lane_block(rows):
    return lax.broadcasted_iota(jnp.int32, (rows, HALF), 1) // NF


def turned(row, k):
    lane = lax.broadcasted_iota(jnp.int32, row.shape, 1)
    near = pltpu.roll(row, 256 - k * NF, 1)
    far = pltpu.roll(row, HALF - k * NF, 1)
    return jnp.where(lane < HALF - k * NF, near, far)


def middle_kernel(w_ref, x_ref, p_ref, s_ref, out_ref, part_ref, sem):
    parts = (p_ref[...] + dot(w_ref[...], rows_of(x_ref))).astype(BF16)
    emit(parts, part_ref)
    save = pltpu.make_async_copy(part_ref, s_ref.at[:, pl.ds(0, parts.shape[1])], sem)
    save.start()
    out_ref[...] = gram_of(parts)
    save.wait()


def middle(w, x, p, pts):
    times = w.shape[1]
    width = x.shape[2]
    here = pl.BlockSpec(memory_space=pltpu.VMEM)
    return pl.pallas_call(
        middle_kernel,
        out_shape=(
            jax.ShapeDtypeStruct((ROWS, pts), BF16),
            jax.ShapeDtypeStruct((ROWS, HALF), F32),
            jax.ShapeDtypeStruct((ROWS, width), BF16),
        ),
        in_specs=[here] * 3,
        out_specs=(pl.BlockSpec(memory_space=pl.ANY), here, here),
        scratch_shapes=[pltpu.SemaphoreType.DMA],
        compiler_params=pltpu.CompilerParams(vmem_limit_bytes=16 * 2**20),
        cost_estimate=pl.CostEstimate(flops=2 * ROWS * times * width, bytes_accessed=2**22, transcendentals=0),
        name="middle",
    )(w, x, p)


def rest_kernel(low, w_ref, x_ref, p_ref, g0_ref, g1_ref, _, s_ref, t_ref, part_ref, row_ref, sem):
    width = x_ref.shape[2]
    parts = (p_ref[...] + dot(w_ref[...], rows_of(x_ref))).astype(BF16)
    emit(parts, part_ref)
    save = pltpu.make_async_copy(part_ref, s_ref.at[:, pl.ds(low, width)], sem)
    save.start()
    kept = jnp.where(same_freq(ROWS), g0_ref[...] + g1_ref[...] + gram_of(parts), 0.0)
    tables = kept.reshape(2 * NB, NF, HALF).sum(axis=1)
    block = lax.broadcasted_iota(jnp.int32, (NB, HALF), 0)
    row_ref[...] = jnp.zeros_like(row_ref)
    for k in range(NB):
        pick = (lane_block(NB) + k) % NB == block
        if k <= PAIRS:
            row_ref[k : k + 1, :HALF] = jnp.where(pick, tables[:NB], 0.0).sum(axis=0, keepdims=True)
        if k:
            row_ref[NB + k : NB + k + 1, :HALF] = jnp.where(pick, tables[NB:], 0.0).sum(axis=0, keepdims=True)
    rows = [row_ref[k : k + 1, :] for k in range(2 * NB)]
    imag = [rows[NB + k] - turned(rows[2 * NB - k], k) for k in range(1, PAIRS + 1)]
    sums = jnp.concatenate(rows[: PAIRS + 1] + imag + [jnp.zeros_like(imag[0])], axis=0)
    for i in range(t_ref.shape[0]):
        t_ref[i] = sums
    save.wait()


def rest(w, x, p, g0, g1, s, low, copies):
    times = w.shape[1]
    width = x.shape[2]
    here = pl.BlockSpec(memory_space=pltpu.VMEM)
    there = pl.BlockSpec(memory_space=pl.ANY)
    return pl.pallas_call(
        functools.partial(rest_kernel, low),
        out_shape=(
            jax.ShapeDtypeStruct(s.shape, BF16),
            jax.ShapeDtypeStruct((copies, 8, 256), F32),
            jax.ShapeDtypeStruct((ROWS, width), BF16),
        ),
        in_specs=[here] * 5 + [there],
        out_specs=(there, here, here),
        scratch_shapes=[pltpu.VMEM((16, 256), F32), pltpu.SemaphoreType.DMA],
        input_output_aliases={5: 0},
        compiler_params=pltpu.CompilerParams(vmem_limit_bytes=16 * 2**20),
        cost_estimate=pl.CostEstimate(flops=2 * ROWS * times * width, bytes_accessed=2**22, transcendentals=0),
        name="rest",
    )(w, x, p, g0, g1, s)


def spread_to(part):
    row = lax.broadcasted_iota(jnp.int32, (HALF, ROWS), 0)
    col = lax.broadcasted_iota(jnp.int32, (HALF, ROWS), 1)
    return (col == row // NF * 2 * NF + part * NF + row % NF).astype(BF16)


def power_kernel(denominator, t_ref, *refs):
    part_refs, (o_ref, m_ref, out_ref, sem) = refs[:-4], refs[-4:]
    sums = jnp.sum(t_ref[...], axis=0) / denominator
    real_rows = [sums[k : k + 1, :] for k in range(PAIRS + 1)]
    imag_rows = [jnp.zeros_like(real_rows[0])] + [sums[PAIRS + k : PAIRS + k + 1, :] for k in range(1, PAIRS + 1)]
    for k in range(PAIRS + 1, NB):
        real_rows.append(turned(real_rows[NB - k], k))
        imag_rows.append(-turned(imag_rows[NB - k], k))
    block = lane_block(1)
    tables = []
    for rows in (real_rows, imag_rows):
        picked = [sum(jnp.where((block + k) % NB == b, rows[k][:, :HALF], 0.0) for k in range(NB)) for b in range(NB)]
        tables.append(jnp.concatenate(picked, axis=0).astype(BF16))
    real, imag = tables
    spread = [spread_to(part) for part in range(2)]
    from_real = dot(real, spread[0]) - dot(imag, spread[1])
    from_imag = dot(imag, spread[0]) + dot(real, spread[1])
    same = lax.broadcasted_iota(jnp.int32, (NF, ROWS), 0) == lax.broadcasted_iota(jnp.int32, (NF, ROWS), 1) % NF
    for b in range(NB):
        for part, table in enumerate((from_real, from_imag)):
            at = (2 * b + part) * NF
            row = jnp.broadcast_to(table[b : b + 1], (NF, ROWS))
            m_ref[at : at + NF, :] = jnp.where(same, row, 0.0).astype(BF16)
    stores = []
    low = 0
    for part_ref in part_refs:
        for at in range(0, part_ref.shape[1], 512):
            values = part_ref[:, at : at + 512]
            cols = pl.ds(low, values.shape[1])
            out_ref[:, low : low + values.shape[1]] = dot(m_ref[...], values)
            stores.append(pltpu.make_async_copy(out_ref.at[:, cols], o_ref.at[:, cols], sem.at[len(stores)]))
            stores[-1].start()
            low += values.shape[1]
    for store in stores:
        store.wait()


def power(t, parts, denominator):
    pts = sum(part.shape[1] for part in parts)
    here = pl.BlockSpec(memory_space=pltpu.VMEM)
    return pl.pallas_call(
        functools.partial(power_kernel, denominator),
        out_shape=jax.ShapeDtypeStruct((ROWS, pts), F32),
        in_specs=[here] * (1 + len(parts)),
        out_specs=pl.BlockSpec(memory_space=pl.ANY),
        scratch_shapes=[
            pltpu.VMEM((ROWS, ROWS), BF16),
            pltpu.VMEM((ROWS, pts), F32),
            pltpu.SemaphoreType.DMA((8,)),
        ],
        compiler_params=pltpu.CompilerParams(vmem_limit_bytes=16 * 2**20),
        name="power",
    )(t, *parts)


def to_all(t, axes):
    copies = jnp.broadcast_to(t[None], (lax.axis_size(axes), *t.shape))
    return lax.all_to_all(copies, axes, 0, 0, tiled=True)


def exchange(x, axes):
    return lax.all_to_all(x, axes, 0, 0, tiled=True)


def shards(snapshots, block_starts, kept_freqs):
    count = lax.axis_size(TA)
    local = snapshots.shape[0]
    own = snapshots.shape[2] // count
    total = own * count * lax.axis_size("zl")
    swap = [(0, 1), (1, 0)]
    x = snapshots.reshape(local, own * count)

    later = own - FIRST
    low = later - LAST
    (first,) = pack(x, own, [(1, later, FIRST)])
    first = lax.ppermute(first, "zh", swap)
    (pass_on,) = pack(x, own, [(1, 0, later)])
    pass_on = exchange(pass_on, PLANE)
    passed = lax.ppermute(pass_on[:, :, :low], "zh", swap)
    last = lax.ppermute(pass_on[:, :, low:], "zh", swap)
    (mine,) = pack(x, own, [(0, 0, own)])
    x0 = exchange(mine, PLANE)
    side = lax.axis_index("zh")
    place = jnp.arange(local * count // 2, dtype=jnp.int32)
    times = place // 128 * 256 + place % 128
    w0 = weights(block_starts, kept_freqs, times + side * 128)
    w1 = weights(block_starts, kept_freqs, times + (1 - side) * 128)
    first, w0, w1 = lax.optimization_barrier((first, w0, w1))
    first = exchange(first, PLANE)
    p0, p1 = partial(w0, x0, (low, LAST))
    s, g0, part0 = middle(w1, passed, p0, own)
    s, g1, part2 = whole(w0, w1, x0, first, s)
    s, t, part1 = rest(w1, last, p1, g0, g1, s, low, lax.axis_size(("y", "x")))
    t = exchange(t, ("y", "x")).sum(axis=0)
    t = to_all(t, ("zh", "zl", "c"))
    out = power(t, (part0, part1, part2), float(NB * total))
    shape = (1, NB, 2, NF, own)
    return s.reshape(shape), out.reshape(shape)


def solution(mesh):
    split = Mesh(mesh.devices.reshape(4, 2, 4, 2, mesh.shape["ga"]), ("y", "zh", "x", "c", "zl"))
    out = P("zl", None, None, None, TA)
    return jax.shard_map(
        shards, mesh=split, in_specs=(P(TA, "zl", None), P(), P()), out_specs=(out, out), check_vma=False
    )
```

```python
import functools
import math

import jax
import jax.numpy as jnp
from jax import lax
from jax.experimental import pallas as pl
from jax.experimental.pallas import tpu as pltpu
from jax.sharding import Mesh
from jax.sharding import PartitionSpec as P


NFFT = 256
NB = 7
NF = 32
HALF = NB * NF
ROWS = 2 * HALF
PAIRS = NB // 2
TA = ("y", "zh", "x", "c")
PLANE = ("y", "x", "c")
FIRST = 768
LAST = 512
F32 = jnp.float32
BF16 = jnp.bfloat16


def weights(block_starts, kept_freqs, times):
    offset = times[None, :] - block_starts[:, None]
    inside = (offset >= 0) & (offset < NFFT)
    window = 0.5 - 0.5 * jnp.cos(2.0 * math.pi / NFFT * offset.astype(F32))
    scale = jnp.where(inside, window, 0.0)
    phase = kept_freqs[None, :, None] * jnp.where(inside, offset, 0)[:, None, :] % NFFT
    angle = 2.0 * math.pi / NFFT * phase.astype(F32)
    norm = 2.0 / math.sqrt(NFFT)
    real = scale[:, None, :] * jnp.cos(angle) * norm
    imag = -scale[:, None, :] * jnp.sin(angle) * norm
    table = jnp.stack([real, imag]).astype(BF16)
    return table.reshape(ROWS, times.shape[0])


def dot(a, b):
    return jnp.dot(a, b, preferred_element_type=F32)


def dot_t(a, b):
    return lax.dot_general(a, b, (((1,), (1,)), ((), ())), preferred_element_type=F32)


def same_freq(rows):
    row = lax.broadcasted_iota(jnp.int32, (rows, HALF), 0)
    col = lax.broadcasted_iota(jnp.int32, (rows, HALF), 1)
    return row % NF == col % NF


def pack_kernel(own, shift, low, x_ref, out_ref, buffer, in_sem, out_sem):
    side = (lax.axis_index("zh") + shift) % 2
    loads = []
    for d in range(buffer.shape[0]):
        start = ((d // 8) * 16 + d % 8) * own + low + side * (8 * own)
        cols = pl.ds(pl.multiple_of(start, 128), buffer.shape[2])
        loads.append(pltpu.make_async_copy(x_ref.at[:, cols], buffer.at[d], in_sem.at[d]))
        loads[d].start()
    stores = []
    for i in range(len(loads) // 8):
        for load in loads[8 * i : 8 * i + 8]:
            load.wait()
        rows = pl.ds(8 * i, 8)
        stores.append(pltpu.make_async_copy(buffer.at[rows], out_ref.at[rows], out_sem.at[i]))
        stores[i].start()
    for store in stores:
        store.wait()


def pack(x, own, shift, low, pts):
    count = x.shape[1] // own // 2
    shape = (count, x.shape[0], pts)
    return pl.pallas_call(
        functools.partial(pack_kernel, own, shift, low),
        out_shape=jax.ShapeDtypeStruct(shape, x.dtype),
        in_specs=[pl.BlockSpec(memory_space=pltpu.HBM)],
        out_specs=pl.BlockSpec(memory_space=pltpu.HBM),
        scratch_shapes=[
            pltpu.VMEM(shape, x.dtype),
            pltpu.SemaphoreType.DMA((count,)),
            pltpu.SemaphoreType.DMA((count // 8,)),
        ],
        compiler_params=pltpu.CompilerParams(vmem_limit_bytes=60 * 2**20),
        name="pack",
    )(x)


def emit(parts, s_ref):
    for part in range(2):
        for b in range(NB):
            start = part * HALF + b * NF
            s_ref[b * 2 * NF + part * NF : b * 2 * NF + (part + 1) * NF, :] = parts[start : start + NF]


def gram_of(parts):
    real, imag = parts[:HALF], parts[HALF:]
    return jnp.concatenate([dot_t(real, real) + dot_t(imag, imag), dot_t(imag, real)], axis=0)


def rows_of(ref):
    return ref[...].reshape(-1, ref.shape[2])


def whole_kernel(w0_ref, w1_ref, x0_ref, x1_ref, _, s_ref, out_ref, part_ref, sem):
    count = x1_ref.shape[2]
    low = x0_ref.shape[2] - count
    near = x0_ref[:, :, low:].reshape(-1, count)
    parts = (dot(w0_ref[...], near) + dot(w1_ref[...], rows_of(x1_ref))).astype(BF16)
    emit(parts, part_ref)
    save = pltpu.make_async_copy(part_ref, s_ref.at[:, pl.ds(low, count)], sem)
    save.start()
    out_ref[...] = gram_of(parts)
    save.wait()


def whole(w0, w1, x0, x1, s):
    times = w0.shape[1]
    count = x1.shape[2]
    here = pl.BlockSpec(memory_space=pltpu.VMEM)
    there = pl.BlockSpec(memory_space=pl.ANY)
    return pl.pallas_call(
        whole_kernel,
        out_shape=(
            jax.ShapeDtypeStruct(s.shape, BF16),
            jax.ShapeDtypeStruct((ROWS, HALF), F32),
            jax.ShapeDtypeStruct((ROWS, count), BF16),
        ),
        in_specs=[here] * 4 + [there],
        out_specs=(there, here, here),
        scratch_shapes=[pltpu.SemaphoreType.DMA],
        input_output_aliases={4: 0},
        compiler_params=pltpu.CompilerParams(vmem_limit_bytes=16 * 2**20),
        cost_estimate=pl.CostEstimate(flops=4 * ROWS * times * count, bytes_accessed=2**22, transcendentals=0),
        name="whole",
    )(w0, w1, x0, x1, s)


def partial_kernel(w_ref, x_ref, *p_refs):
    low = 0
    for p_ref in p_refs:
        count = p_ref.shape[1]
        p_ref[...] = dot(w_ref[...], x_ref[:, :, low : low + count].reshape(-1, count))
        low += count


def partial(w, x, counts):
    times = w.shape[1]
    here = pl.BlockSpec(memory_space=pltpu.VMEM)
    return pl.pallas_call(
        partial_kernel,
        out_shape=[jax.ShapeDtypeStruct((ROWS, count), F32) for count in counts],
        in_specs=[here, here],
        out_specs=[here] * len(counts),
        compiler_params=pltpu.CompilerParams(vmem_limit_bytes=16 * 2**20),
        cost_estimate=pl.CostEstimate(flops=2 * ROWS * times * sum(counts), bytes_accessed=2**21, transcendentals=0),
        name="partial",
    )(w, x)


def lane_block(rows):
    return lax.broadcasted_iota(jnp.int32, (rows, HALF), 1) // NF


def turned(row, k):
    lane = lax.broadcasted_iota(jnp.int32, row.shape, 1)
    near = pltpu.roll(row, 256 - k * NF, 1)
    far = pltpu.roll(row, HALF - k * NF, 1)
    return jnp.where(lane < HALF - k * NF, near, far)


def middle_kernel(w_ref, x_ref, p_ref, s_ref, out_ref, part_ref, sem):
    parts = (p_ref[...] + dot(w_ref[...], rows_of(x_ref))).astype(BF16)
    emit(parts, part_ref)
    save = pltpu.make_async_copy(part_ref, s_ref.at[:, pl.ds(0, parts.shape[1])], sem)
    save.start()
    out_ref[...] = gram_of(parts)
    save.wait()


def middle(w, x, p, pts):
    times = w.shape[1]
    width = x.shape[2]
    here = pl.BlockSpec(memory_space=pltpu.VMEM)
    return pl.pallas_call(
        middle_kernel,
        out_shape=(
            jax.ShapeDtypeStruct((ROWS, pts), BF16),
            jax.ShapeDtypeStruct((ROWS, HALF), F32),
            jax.ShapeDtypeStruct((ROWS, width), BF16),
        ),
        in_specs=[here] * 3,
        out_specs=(pl.BlockSpec(memory_space=pl.ANY), here, here),
        scratch_shapes=[pltpu.SemaphoreType.DMA],
        compiler_params=pltpu.CompilerParams(vmem_limit_bytes=16 * 2**20),
        cost_estimate=pl.CostEstimate(flops=2 * ROWS * times * width, bytes_accessed=2**22, transcendentals=0),
        name="middle",
    )(w, x, p)


def rest_kernel(low, w_ref, x_ref, p_ref, g0_ref, g1_ref, _, s_ref, t_ref, part_ref, row_ref, sem):
    width = x_ref.shape[2]
    parts = (p_ref[...] + dot(w_ref[...], rows_of(x_ref))).astype(BF16)
    emit(parts, part_ref)
    save = pltpu.make_async_copy(part_ref, s_ref.at[:, pl.ds(low, width)], sem)
    save.start()
    kept = jnp.where(same_freq(ROWS), g0_ref[...] + g1_ref[...] + gram_of(parts), 0.0)
    tables = kept.reshape(2 * NB, NF, HALF).sum(axis=1)
    block = lax.broadcasted_iota(jnp.int32, (NB, HALF), 0)
    row_ref[...] = jnp.zeros_like(row_ref)
    for k in range(NB):
        pick = (lane_block(NB) + k) % NB == block
        if k <= PAIRS:
            row_ref[k : k + 1, :HALF] = jnp.where(pick, tables[:NB], 0.0).sum(axis=0, keepdims=True)
        if k:
            row_ref[NB + k : NB + k + 1, :HALF] = jnp.where(pick, tables[NB:], 0.0).sum(axis=0, keepdims=True)
    rows = [row_ref[k : k + 1, :] for k in range(2 * NB)]
    imag = [rows[NB + k] - turned(rows[2 * NB - k], k) for k in range(1, PAIRS + 1)]
    sums = jnp.concatenate(rows[: PAIRS + 1] + imag + [jnp.zeros_like(imag[0])], axis=0)
    for i in range(t_ref.shape[0]):
        t_ref[i] = sums
    save.wait()


def rest(w, x, p, g0, g1, s, low, copies):
    times = w.shape[1]
    width = x.shape[2]
    here = pl.BlockSpec(memory_space=pltpu.VMEM)
    there = pl.BlockSpec(memory_space=pl.ANY)
    return pl.pallas_call(
        functools.partial(rest_kernel, low),
        out_shape=(
            jax.ShapeDtypeStruct(s.shape, BF16),
            jax.ShapeDtypeStruct((copies, 8, 256), F32),
            jax.ShapeDtypeStruct((ROWS, width), BF16),
        ),
        in_specs=[here] * 5 + [there],
        out_specs=(there, here, here),
        scratch_shapes=[pltpu.VMEM((16, 256), F32), pltpu.SemaphoreType.DMA],
        input_output_aliases={5: 0},
        compiler_params=pltpu.CompilerParams(vmem_limit_bytes=16 * 2**20),
        cost_estimate=pl.CostEstimate(flops=2 * ROWS * times * width, bytes_accessed=2**22, transcendentals=0),
        name="rest",
    )(w, x, p, g0, g1, s)


def spread_to(part):
    row = lax.broadcasted_iota(jnp.int32, (HALF, ROWS), 0)
    col = lax.broadcasted_iota(jnp.int32, (HALF, ROWS), 1)
    return (col == row // NF * 2 * NF + part * NF + row % NF).astype(BF16)


def power_kernel(denominator, t_ref, *refs):
    part_refs, (o_ref, m_ref, out_ref, sem) = refs[:-4], refs[-4:]
    sums = jnp.sum(t_ref[...].astype(F32), axis=0) / denominator
    real_rows = [sums[k : k + 1, :] for k in range(PAIRS + 1)]
    imag_rows = [jnp.zeros_like(real_rows[0])] + [sums[PAIRS + k : PAIRS + k + 1, :] for k in range(1, PAIRS + 1)]
    for k in range(PAIRS + 1, NB):
        real_rows.append(turned(real_rows[NB - k], k))
        imag_rows.append(-turned(imag_rows[NB - k], k))
    block = lane_block(1)
    tables = []
    for rows in (real_rows, imag_rows):
        picked = [sum(jnp.where((block + k) % NB == b, rows[k][:, :HALF], 0.0) for k in range(NB)) for b in range(NB)]
        tables.append(jnp.concatenate(picked, axis=0).astype(BF16))
    real, imag = tables
    spread = [spread_to(part) for part in range(2)]
    from_real = dot(real, spread[0]) - dot(imag, spread[1])
    from_imag = dot(imag, spread[0]) + dot(real, spread[1])
    same = lax.broadcasted_iota(jnp.int32, (NF, ROWS), 0) == lax.broadcasted_iota(jnp.int32, (NF, ROWS), 1) % NF
    for b in range(NB):
        for part, table in enumerate((from_real, from_imag)):
            at = (2 * b + part) * NF
            row = jnp.broadcast_to(table[b : b + 1], (NF, ROWS))
            m_ref[at : at + NF, :] = jnp.where(same, row, 0.0).astype(BF16)
    stores = []
    low = 0
    for part_ref in part_refs:
        for at in range(0, part_ref.shape[1], 512):
            values = part_ref[:, at : at + 512]
            cols = pl.ds(low, values.shape[1])
            out_ref[:, low : low + values.shape[1]] = dot(m_ref[...], values)
            stores.append(pltpu.make_async_copy(out_ref.at[:, cols], o_ref.at[:, cols], sem.at[len(stores)]))
            stores[-1].start()
            low += values.shape[1]
    for store in stores:
        store.wait()


def power(t, parts, denominator):
    pts = sum(part.shape[1] for part in parts)
    here = pl.BlockSpec(memory_space=pltpu.VMEM)
    return pl.pallas_call(
        functools.partial(power_kernel, denominator),
        out_shape=jax.ShapeDtypeStruct((ROWS, pts), F32),
        in_specs=[here] * (1 + len(parts)),
        out_specs=pl.BlockSpec(memory_space=pl.ANY),
        scratch_shapes=[
            pltpu.VMEM((ROWS, ROWS), BF16),
            pltpu.VMEM((ROWS, pts), F32),
            pltpu.SemaphoreType.DMA((8,)),
        ],
        compiler_params=pltpu.CompilerParams(vmem_limit_bytes=16 * 2**20),
        name="power",
    )(t, *parts)


def to_all(t, axes):
    copies = jnp.broadcast_to(t[None], (lax.axis_size(axes), *t.shape))
    return lax.all_to_all(copies, axes, 0, 0, tiled=True)


def exchange(x, axes):
    return lax.all_to_all(x, axes, 0, 0, tiled=True)


def shards(snapshots, block_starts, kept_freqs):
    count = lax.axis_size(TA)
    local = snapshots.shape[0]
    own = snapshots.shape[2] // count
    total = own * count * lax.axis_size("zl")
    swap = [(0, 1), (1, 0)]
    x = snapshots.reshape(local, own * count)

    later = own - FIRST
    low = later - LAST
    first = pack(x, own, 1, later, FIRST)
    first = lax.ppermute(first, "zh", swap)
    pass_on = pack(x, own, 1, 0, later)
    pass_on = exchange(pass_on, PLANE)
    passed = lax.ppermute(pass_on[:, :, :low], "zh", swap)
    last = lax.ppermute(pass_on[:, :, low:], "zh", swap)
    mine = pack(x, own, 0, 0, own)
    x0 = exchange(mine, PLANE)
    side = lax.axis_index("zh")
    place = jnp.arange(local * count // 2, dtype=jnp.int32)
    times = place // 128 * 256 + place % 128
    w0 = weights(block_starts, kept_freqs, times + side * 128)
    w1 = weights(block_starts, kept_freqs, times + (1 - side) * 128)
    first, w0, w1 = lax.optimization_barrier((first, w0, w1))
    first = exchange(first, PLANE)
    p0, p1 = partial(w0, x0, (low, LAST))
    s, g0, part0 = middle(w1, passed, p0, own)
    s, g1, part2 = whole(w0, w1, x0, first, s)
    s, t, part1 = rest(w1, last, p1, g0, g1, s, low, lax.axis_size(("y", "x")))
    t = exchange(t, ("y", "x")).sum(axis=0)
    t = to_all(t.astype(BF16), ("zh", "zl", "c"))
    out = power(t, (part0, part1, part2), float(NB * total))
    shape = (1, NB, 2, NF, own)
    return s.reshape(shape), out.reshape(shape)


def solution(mesh):
    split = Mesh(mesh.devices.reshape(4, 2, 4, 2, mesh.shape["ga"]), ("y", "zh", "x", "c", "zl"))
    out = P("zl", None, None, None, TA)
    return jax.shard_map(
        shards, mesh=split, in_specs=(P(TA, "zl", None), P(), P()), out_specs=(out, out), check_vma=False
    )
```

```python
import functools
import math

import jax
import jax.numpy as jnp
from jax import lax
from jax.experimental import pallas as pl
from jax.experimental.pallas import tpu as pltpu
from jax.sharding import Mesh
from jax.sharding import PartitionSpec as P


NFFT = 256
NB = 7
NF = 32
HALF = NB * NF
ROWS = 2 * HALF
PAIRS = NB // 2
TA = ("y", "zh", "x", "c")
PLANE = ("y", "x", "c")
FIRST = 768
LAST = 256
F32 = jnp.float32
BF16 = jnp.bfloat16


def weights(block_starts, kept_freqs, times):
    offset = times[None, :] - block_starts[:, None]
    inside = (offset >= 0) & (offset < NFFT)
    window = 0.5 - 0.5 * jnp.cos(2.0 * math.pi / NFFT * offset.astype(F32))
    scale = jnp.where(inside, window, 0.0)
    phase = kept_freqs[None, :, None] * jnp.where(inside, offset, 0)[:, None, :] % NFFT
    angle = 2.0 * math.pi / NFFT * phase.astype(F32)
    norm = 2.0 / math.sqrt(NFFT)
    real = scale[:, None, :] * jnp.cos(angle) * norm
    imag = -scale[:, None, :] * jnp.sin(angle) * norm
    table = jnp.stack([real, imag]).astype(BF16)
    return table.reshape(ROWS, times.shape[0])


def dot(a, b):
    return jnp.dot(a, b, preferred_element_type=F32)


def dot_t(a, b):
    return lax.dot_general(a, b, (((1,), (1,)), ((), ())), preferred_element_type=F32)


def same_freq(rows):
    row = lax.broadcasted_iota(jnp.int32, (rows, HALF), 0)
    col = lax.broadcasted_iota(jnp.int32, (rows, HALF), 1)
    return row % NF == col % NF


def pack_kernel(own, shift, low, x_ref, out_ref, buffer, in_sem, out_sem):
    side = (lax.axis_index("zh") + shift) % 2
    loads = []
    for d in range(buffer.shape[0]):
        start = ((d // 8) * 16 + d % 8) * own + low + side * (8 * own)
        cols = pl.ds(pl.multiple_of(start, 128), buffer.shape[2])
        loads.append(pltpu.make_async_copy(x_ref.at[:, cols], buffer.at[d], in_sem.at[d]))
        loads[d].start()
    stores = []
    for i in range(len(loads) // 8):
        for load in loads[8 * i : 8 * i + 8]:
            load.wait()
        rows = pl.ds(8 * i, 8)
        stores.append(pltpu.make_async_copy(buffer.at[rows], out_ref.at[rows], out_sem.at[i]))
        stores[i].start()
    for store in stores:
        store.wait()


def pack(x, own, shift, low, pts):
    count = x.shape[1] // own // 2
    shape = (count, x.shape[0], pts)
    return pl.pallas_call(
        functools.partial(pack_kernel, own, shift, low),
        out_shape=jax.ShapeDtypeStruct(shape, x.dtype),
        in_specs=[pl.BlockSpec(memory_space=pltpu.HBM)],
        out_specs=pl.BlockSpec(memory_space=pltpu.HBM),
        scratch_shapes=[
            pltpu.VMEM(shape, x.dtype),
            pltpu.SemaphoreType.DMA((count,)),
            pltpu.SemaphoreType.DMA((count // 8,)),
        ],
        compiler_params=pltpu.CompilerParams(vmem_limit_bytes=60 * 2**20),
        name="pack",
    )(x)


def emit(parts, s_ref):
    for part in range(2):
        for b in range(NB):
            start = part * HALF + b * NF
            s_ref[b * 2 * NF + part * NF : b * 2 * NF + (part + 1) * NF, :] = parts[start : start + NF]


def gram_of(parts):
    real, imag = parts[:HALF], parts[HALF:]
    return jnp.concatenate([dot_t(real, real) + dot_t(imag, imag), dot_t(imag, real)], axis=0)


def rows_of(ref):
    return ref[...].reshape(-1, ref.shape[2])


def whole_kernel(w0_ref, w1_ref, x0_ref, x1_ref, _, s_ref, out_ref, part_ref, sem):
    count = x1_ref.shape[2]
    low = x0_ref.shape[2] - count
    near = x0_ref[:, :, low:].reshape(-1, count)
    parts = (dot(w0_ref[...], near) + dot(w1_ref[...], rows_of(x1_ref))).astype(BF16)
    emit(parts, part_ref)
    save = pltpu.make_async_copy(part_ref, s_ref.at[:, pl.ds(low, count)], sem)
    save.start()
    out_ref[...] = gram_of(parts)
    save.wait()


def whole(w0, w1, x0, x1, s):
    times = w0.shape[1]
    count = x1.shape[2]
    here = pl.BlockSpec(memory_space=pltpu.VMEM)
    there = pl.BlockSpec(memory_space=pl.ANY)
    return pl.pallas_call(
        whole_kernel,
        out_shape=(
            jax.ShapeDtypeStruct(s.shape, BF16),
            jax.ShapeDtypeStruct((ROWS, HALF), F32),
            jax.ShapeDtypeStruct((ROWS, count), BF16),
        ),
        in_specs=[here] * 4 + [there],
        out_specs=(there, here, here),
        scratch_shapes=[pltpu.SemaphoreType.DMA],
        input_output_aliases={4: 0},
        compiler_params=pltpu.CompilerParams(vmem_limit_bytes=16 * 2**20),
        cost_estimate=pl.CostEstimate(flops=4 * ROWS * times * count, bytes_accessed=2**22, transcendentals=0),
        name="whole",
    )(w0, w1, x0, x1, s)


def partial_kernel(w_ref, x_ref, *p_refs):
    low = 0
    for p_ref in p_refs:
        count = p_ref.shape[1]
        p_ref[...] = dot(w_ref[...], x_ref[:, :, low : low + count].reshape(-1, count))
        low += count


def partial(w, x, counts):
    times = w.shape[1]
    here = pl.BlockSpec(memory_space=pltpu.VMEM)
    return pl.pallas_call(
        partial_kernel,
        out_shape=[jax.ShapeDtypeStruct((ROWS, count), F32) for count in counts],
        in_specs=[here, here],
        out_specs=[here] * len(counts),
        compiler_params=pltpu.CompilerParams(vmem_limit_bytes=16 * 2**20),
        cost_estimate=pl.CostEstimate(flops=2 * ROWS * times * sum(counts), bytes_accessed=2**21, transcendentals=0),
        name="partial",
    )(w, x)


def lane_block(rows):
    return lax.broadcasted_iota(jnp.int32, (rows, HALF), 1) // NF


def turned(row, k):
    lane = lax.broadcasted_iota(jnp.int32, row.shape, 1)
    near = pltpu.roll(row, 256 - k * NF, 1)
    far = pltpu.roll(row, HALF - k * NF, 1)
    return jnp.where(lane < HALF - k * NF, near, far)


def middle_kernel(w_ref, x_ref, p_ref, s_ref, out_ref, part_ref, sem):
    parts = (p_ref[...] + dot(w_ref[...], rows_of(x_ref))).astype(BF16)
    emit(parts, part_ref)
    save = pltpu.make_async_copy(part_ref, s_ref.at[:, pl.ds(0, parts.shape[1])], sem)
    save.start()
    out_ref[...] = gram_of(parts)
    save.wait()


def middle(w, x, p, pts):
    times = w.shape[1]
    width = x.shape[2]
    here = pl.BlockSpec(memory_space=pltpu.VMEM)
    return pl.pallas_call(
        middle_kernel,
        out_shape=(
            jax.ShapeDtypeStruct((ROWS, pts), BF16),
            jax.ShapeDtypeStruct((ROWS, HALF), F32),
            jax.ShapeDtypeStruct((ROWS, width), BF16),
        ),
        in_specs=[here] * 3,
        out_specs=(pl.BlockSpec(memory_space=pl.ANY), here, here),
        scratch_shapes=[pltpu.SemaphoreType.DMA],
        compiler_params=pltpu.CompilerParams(vmem_limit_bytes=16 * 2**20),
        cost_estimate=pl.CostEstimate(flops=2 * ROWS * times * width, bytes_accessed=2**22, transcendentals=0),
        name="middle",
    )(w, x, p)


def rest_kernel(low, w_ref, x_ref, p_ref, g0_ref, g1_ref, _, s_ref, t_ref, part_ref, row_ref, sem):
    width = x_ref.shape[2]
    parts = (p_ref[...] + dot(w_ref[...], rows_of(x_ref))).astype(BF16)
    emit(parts, part_ref)
    save = pltpu.make_async_copy(part_ref, s_ref.at[:, pl.ds(low, width)], sem)
    save.start()
    kept = jnp.where(same_freq(ROWS), g0_ref[...] + g1_ref[...] + gram_of(parts), 0.0)
    tables = kept.reshape(2 * NB, NF, HALF).sum(axis=1)
    block = lax.broadcasted_iota(jnp.int32, (NB, HALF), 0)
    row_ref[...] = jnp.zeros_like(row_ref)
    for k in range(NB):
        pick = (lane_block(NB) + k) % NB == block
        if k <= PAIRS:
            row_ref[k : k + 1, :HALF] = jnp.where(pick, tables[:NB], 0.0).sum(axis=0, keepdims=True)
        if k:
            row_ref[NB + k : NB + k + 1, :HALF] = jnp.where(pick, tables[NB:], 0.0).sum(axis=0, keepdims=True)
    rows = [row_ref[k : k + 1, :] for k in range(2 * NB)]
    imag = [rows[NB + k] - turned(rows[2 * NB - k], k) for k in range(1, PAIRS + 1)]
    sums = jnp.concatenate(rows[: PAIRS + 1] + imag + [jnp.zeros_like(imag[0])], axis=0)
    for i in range(t_ref.shape[0]):
        t_ref[i] = sums
    save.wait()


def rest(w, x, p, g0, g1, s, low, copies):
    times = w.shape[1]
    width = x.shape[2]
    here = pl.BlockSpec(memory_space=pltpu.VMEM)
    there = pl.BlockSpec(memory_space=pl.ANY)
    return pl.pallas_call(
        functools.partial(rest_kernel, low),
        out_shape=(
            jax.ShapeDtypeStruct(s.shape, BF16),
            jax.ShapeDtypeStruct((copies, 8, 256), F32),
            jax.ShapeDtypeStruct((ROWS, width), BF16),
        ),
        in_specs=[here] * 5 + [there],
        out_specs=(there, here, here),
        scratch_shapes=[pltpu.VMEM((16, 256), F32), pltpu.SemaphoreType.DMA],
        input_output_aliases={5: 0},
        compiler_params=pltpu.CompilerParams(vmem_limit_bytes=16 * 2**20),
        cost_estimate=pl.CostEstimate(flops=2 * ROWS * times * width, bytes_accessed=2**22, transcendentals=0),
        name="rest",
    )(w, x, p, g0, g1, s)


def spread_to(part):
    row = lax.broadcasted_iota(jnp.int32, (HALF, ROWS), 0)
    col = lax.broadcasted_iota(jnp.int32, (HALF, ROWS), 1)
    return (col == row // NF * 2 * NF + part * NF + row % NF).astype(BF16)


def power_kernel(denominator, lows, t_ref, *refs):
    part_refs, (o_ref, m_ref, out_ref, sem) = refs[:-4], refs[-4:]
    sums = jnp.sum(t_ref[...].astype(F32), axis=0) / denominator
    real_rows = [sums[k : k + 1, :] for k in range(PAIRS + 1)]
    imag_rows = [jnp.zeros_like(real_rows[0])] + [sums[PAIRS + k : PAIRS + k + 1, :] for k in range(1, PAIRS + 1)]
    for k in range(PAIRS + 1, NB):
        real_rows.append(turned(real_rows[NB - k], k))
        imag_rows.append(-turned(imag_rows[NB - k], k))
    block = lane_block(1)
    tables = []
    for rows in (real_rows, imag_rows):
        picked = [sum(jnp.where((block + k) % NB == b, rows[k][:, :HALF], 0.0) for k in range(NB)) for b in range(NB)]
        tables.append(jnp.concatenate(picked, axis=0).astype(BF16))
    real, imag = tables
    spread = [spread_to(part) for part in range(2)]
    from_real = dot(real, spread[0]) - dot(imag, spread[1])
    from_imag = dot(imag, spread[0]) + dot(real, spread[1])
    same = lax.broadcasted_iota(jnp.int32, (NF, ROWS), 0) == lax.broadcasted_iota(jnp.int32, (NF, ROWS), 1) % NF
    for b in range(NB):
        for part, table in enumerate((from_real, from_imag)):
            at = (2 * b + part) * NF
            row = jnp.broadcast_to(table[b : b + 1], (NF, ROWS))
            m_ref[at : at + NF, :] = jnp.where(same, row, 0.0).astype(BF16)
    stores = []
    for low, part_ref in zip(lows, part_refs):
        for at in range(0, part_ref.shape[1], 512):
            values = part_ref[:, at : at + 512]
            cols = pl.ds(low, values.shape[1])
            out_ref[:, low : low + values.shape[1]] = dot(m_ref[...], values)
            stores.append(pltpu.make_async_copy(out_ref.at[:, cols], o_ref.at[:, cols], sem.at[len(stores)]))
            stores[-1].start()
            low += values.shape[1]
    for store in stores:
        store.wait()


def power(t, parts, lows, denominator):
    pts = sum(part.shape[1] for part in parts)
    here = pl.BlockSpec(memory_space=pltpu.VMEM)
    return pl.pallas_call(
        functools.partial(power_kernel, denominator, lows),
        out_shape=jax.ShapeDtypeStruct((ROWS, pts), F32),
        in_specs=[here] * (1 + len(parts)),
        out_specs=pl.BlockSpec(memory_space=pl.ANY),
        scratch_shapes=[
            pltpu.VMEM((ROWS, ROWS), BF16),
            pltpu.VMEM((ROWS, pts), F32),
            pltpu.SemaphoreType.DMA((8,)),
        ],
        compiler_params=pltpu.CompilerParams(vmem_limit_bytes=16 * 2**20),
        name="power",
    )(t, *parts)


def to_all(t, axes):
    copies = jnp.broadcast_to(t[None], (lax.axis_size(axes), *t.shape))
    return lax.all_to_all(copies, axes, 0, 0, tiled=True)


def exchange(x, axes):
    return lax.all_to_all(x, axes, 0, 0, tiled=True)


def shards(snapshots, block_starts, kept_freqs):
    count = lax.axis_size(TA)
    local = snapshots.shape[0]
    own = snapshots.shape[2] // count
    total = own * count * lax.axis_size("zl")
    swap = [(0, 1), (1, 0)]
    x = snapshots.reshape(local, own * count)

    later = own - FIRST
    low = later - LAST
    first = pack(x, own, 1, later, FIRST)
    first = lax.ppermute(first, "zh", swap)
    pass_on = pack(x, own, 1, 0, later)
    pass_on = exchange(pass_on, PLANE)
    passed = lax.ppermute(pass_on[:, :, :low], "zh", swap)
    last = lax.ppermute(pass_on[:, :, low:], "zh", swap)
    mine = pack(x, own, 0, 0, own)
    x0 = exchange(mine, PLANE)
    side = lax.axis_index("zh")
    place = jnp.arange(local * count // 2, dtype=jnp.int32)
    times = place // 128 * 256 + place % 128
    w0 = weights(block_starts, kept_freqs, times + side * 128)
    w1 = weights(block_starts, kept_freqs, times + (1 - side) * 128)
    first, w0, w1 = lax.optimization_barrier((first, w0, w1))
    first = exchange(first, PLANE)
    p0, p1 = partial(w0, x0, (low, LAST))
    s, g0, part0 = middle(w1, passed, p0, own)
    s, g1, part2 = whole(w0, w1, x0, first, s)
    s, t, part1 = rest(w1, last, p1, g0, g1, s, low, lax.axis_size(("y", "x")))
    t = exchange(t, ("y", "x")).sum(axis=0)
    t = to_all(t.astype(BF16), ("zh", "zl", "c"))
    out = power(t, (part1, part0, part2), (low, 0, later), float(NB * total))
    shape = (1, NB, 2, NF, own)
    return s.reshape(shape), out.reshape(shape)


def solution(mesh):
    split = Mesh(mesh.devices.reshape(4, 2, 4, 2, mesh.shape["ga"]), ("y", "zh", "x", "c", "zl"))
    out = P("zl", None, None, None, TA)
    return jax.shard_map(
        shards, mesh=split, in_specs=(P(TA, "zl", None), P(), P()), out_specs=(out, out), check_vma=False
    )
```

```python
import functools
import math

import jax
import jax.numpy as jnp
from jax import lax
from jax.experimental import pallas as pl
from jax.experimental.pallas import tpu as pltpu
from jax.sharding import Mesh
from jax.sharding import PartitionSpec as P


NFFT = 256
NB = 7
NF = 32
HALF = NB * NF
ROWS = 2 * HALF
PAIRS = NB // 2
TA = ("y", "zh", "x", "c")
PLANE = ("y", "x", "c")
FIRST = 768
LAST = 512
F32 = jnp.float32
BF16 = jnp.bfloat16


def weights(block_starts, kept_freqs, times):
    offset = times[None, :] - block_starts[:, None]
    inside = (offset >= 0) & (offset < NFFT)
    window = 0.5 - 0.5 * jnp.cos(2.0 * math.pi / NFFT * offset.astype(F32))
    scale = jnp.where(inside, window, 0.0)
    phase = kept_freqs[None, :, None] * jnp.where(inside, offset, 0)[:, None, :] % NFFT
    angle = 2.0 * math.pi / NFFT * phase.astype(F32)
    norm = 2.0 / math.sqrt(NFFT)
    real = scale[:, None, :] * jnp.cos(angle) * norm
    imag = -scale[:, None, :] * jnp.sin(angle) * norm
    table = jnp.stack([real, imag]).astype(BF16)
    return table.reshape(ROWS, times.shape[0])


def dot(a, b):
    return jnp.dot(a, b, preferred_element_type=F32)


def dot_t(a, b):
    return lax.dot_general(a, b, (((1,), (1,)), ((), ())), preferred_element_type=F32)


def same_freq(rows):
    row = lax.broadcasted_iota(jnp.int32, (rows, HALF), 0)
    col = lax.broadcasted_iota(jnp.int32, (rows, HALF), 1)
    return row % NF == col % NF


def pack_kernel(own, shift, low, x_ref, out_ref, buffer, in_sem, out_sem):
    side = (lax.axis_index("zh") + shift) % 2
    loads = []
    for d in range(buffer.shape[0]):
        start = ((d // 8) * 16 + d % 8) * own + low + side * (8 * own)
        cols = pl.ds(pl.multiple_of(start, 128), buffer.shape[2])
        loads.append(pltpu.make_async_copy(x_ref.at[:, cols], buffer.at[d], in_sem.at[d]))
        loads[d].start()
    stores = []
    for i in range(len(loads) // 8):
        for load in loads[8 * i : 8 * i + 8]:
            load.wait()
        rows = pl.ds(8 * i, 8)
        stores.append(pltpu.make_async_copy(buffer.at[rows], out_ref.at[rows], out_sem.at[i]))
        stores[i].start()
    for store in stores:
        store.wait()


def pack(x, own, shift, low, pts):
    count = x.shape[1] // own // 2
    shape = (count, x.shape[0], pts)
    return pl.pallas_call(
        functools.partial(pack_kernel, own, shift, low),
        out_shape=jax.ShapeDtypeStruct(shape, x.dtype),
        in_specs=[pl.BlockSpec(memory_space=pltpu.HBM)],
        out_specs=pl.BlockSpec(memory_space=pltpu.HBM),
        scratch_shapes=[
            pltpu.VMEM(shape, x.dtype),
            pltpu.SemaphoreType.DMA((count,)),
            pltpu.SemaphoreType.DMA((count // 8,)),
        ],
        compiler_params=pltpu.CompilerParams(vmem_limit_bytes=60 * 2**20),
        name="pack",
    )(x)


def emit(parts, s_ref):
    for part in range(2):
        for b in range(NB):
            start = part * HALF + b * NF
            s_ref[b * 2 * NF + part * NF : b * 2 * NF + (part + 1) * NF, :] = parts[start : start + NF]


def gram_of(parts):
    real, imag = parts[:HALF], parts[HALF:]
    return jnp.concatenate([dot_t(real, real) + dot_t(imag, imag), dot_t(imag, real)], axis=0)


def rows_of(ref):
    return ref[...].reshape(-1, ref.shape[2])


def whole_kernel(w0_ref, w1_ref, x0_ref, x1_ref, _, s_ref, out_ref, part_ref, sem):
    count = x1_ref.shape[2]
    low = x0_ref.shape[2] - count
    near = x0_ref[:, :, low:].reshape(-1, count)
    parts = (dot(w0_ref[...], near) + dot(w1_ref[...], rows_of(x1_ref))).astype(BF16)
    emit(parts, part_ref)
    save = pltpu.make_async_copy(part_ref, s_ref.at[:, pl.ds(low, count)], sem)
    save.start()
    out_ref[...] = gram_of(parts)
    save.wait()


def whole(w0, w1, x0, x1, s):
    times = w0.shape[1]
    count = x1.shape[2]
    here = pl.BlockSpec(memory_space=pltpu.VMEM)
    there = pl.BlockSpec(memory_space=pl.ANY)
    return pl.pallas_call(
        whole_kernel,
        out_shape=(
            jax.ShapeDtypeStruct(s.shape, BF16),
            jax.ShapeDtypeStruct((ROWS, HALF), F32),
            jax.ShapeDtypeStruct((ROWS, count), BF16),
        ),
        in_specs=[here] * 4 + [there],
        out_specs=(there, here, here),
        scratch_shapes=[pltpu.SemaphoreType.DMA],
        input_output_aliases={4: 0},
        compiler_params=pltpu.CompilerParams(vmem_limit_bytes=16 * 2**20),
        cost_estimate=pl.CostEstimate(flops=4 * ROWS * times * count, bytes_accessed=2**22, transcendentals=0),
        name="whole",
    )(w0, w1, x0, x1, s)


def partial_kernel(w_ref, x_ref, *p_refs):
    low = 0
    for p_ref in p_refs:
        count = p_ref.shape[1]
        p_ref[...] = dot(w_ref[...], x_ref[:, :, low : low + count].reshape(-1, count))
        low += count


def partial(w, x, counts):
    times = w.shape[1]
    here = pl.BlockSpec(memory_space=pltpu.VMEM)
    return pl.pallas_call(
        partial_kernel,
        out_shape=[jax.ShapeDtypeStruct((ROWS, count), F32) for count in counts],
        in_specs=[here, here],
        out_specs=[here] * len(counts),
        compiler_params=pltpu.CompilerParams(vmem_limit_bytes=16 * 2**20),
        cost_estimate=pl.CostEstimate(flops=2 * ROWS * times * sum(counts), bytes_accessed=2**21, transcendentals=0),
        name="partial",
    )(w, x)


def lane_block(rows):
    return lax.broadcasted_iota(jnp.int32, (rows, HALF), 1) // NF


def turned(row, k):
    lane = lax.broadcasted_iota(jnp.int32, row.shape, 1)
    near = pltpu.roll(row, 256 - k * NF, 1)
    far = pltpu.roll(row, HALF - k * NF, 1)
    return jnp.where(lane < HALF - k * NF, near, far)


def middle_kernel(w_ref, x_ref, p_ref, s_ref, out_ref, part_ref, sem):
    parts = (p_ref[...] + dot(w_ref[...], rows_of(x_ref))).astype(BF16)
    emit(parts, part_ref)
    save = pltpu.make_async_copy(part_ref, s_ref.at[:, pl.ds(0, parts.shape[1])], sem)
    save.start()
    out_ref[...] = gram_of(parts)
    save.wait()


def middle(w, x, p, pts):
    times = w.shape[1]
    width = x.shape[2]
    here = pl.BlockSpec(memory_space=pltpu.VMEM)
    return pl.pallas_call(
        middle_kernel,
        out_shape=(
            jax.ShapeDtypeStruct((ROWS, pts), BF16),
            jax.ShapeDtypeStruct((ROWS, HALF), F32),
            jax.ShapeDtypeStruct((ROWS, width), BF16),
        ),
        in_specs=[here] * 3,
        out_specs=(pl.BlockSpec(memory_space=pl.ANY), here, here),
        scratch_shapes=[pltpu.SemaphoreType.DMA],
        compiler_params=pltpu.CompilerParams(vmem_limit_bytes=16 * 2**20),
        cost_estimate=pl.CostEstimate(flops=2 * ROWS * times * width, bytes_accessed=2**22, transcendentals=0),
        name="middle",
    )(w, x, p)


def rest_kernel(low, w_ref, x_ref, p_ref, g0_ref, g1_ref, _, s_ref, t_ref, part_ref, row_ref, sem):
    width = x_ref.shape[2]
    parts = (p_ref[...] + dot(w_ref[...], rows_of(x_ref))).astype(BF16)
    emit(parts, part_ref)
    save = pltpu.make_async_copy(part_ref, s_ref.at[:, pl.ds(low, width)], sem)
    save.start()
    kept = jnp.where(same_freq(ROWS), g0_ref[...] + g1_ref[...] + gram_of(parts), 0.0)
    tables = kept.reshape(2 * NB, NF, HALF).sum(axis=1)
    block = lax.broadcasted_iota(jnp.int32, (NB, HALF), 0)
    row_ref[...] = jnp.zeros_like(row_ref)
    for k in range(NB):
        pick = (lane_block(NB) + k) % NB == block
        if k <= PAIRS:
            row_ref[k : k + 1, :HALF] = jnp.where(pick, tables[:NB], 0.0).sum(axis=0, keepdims=True)
        if k:
            row_ref[NB + k : NB + k + 1, :HALF] = jnp.where(pick, tables[NB:], 0.0).sum(axis=0, keepdims=True)
    rows = [row_ref[k : k + 1, :] for k in range(2 * NB)]
    imag = [rows[NB + k] - turned(rows[2 * NB - k], k) for k in range(1, PAIRS + 1)]
    sums = jnp.concatenate(rows[: PAIRS + 1] + imag + [jnp.zeros_like(imag[0])], axis=0)
    for i in range(t_ref.shape[0]):
        t_ref[i] = sums
    save.wait()


def rest(w, x, p, g0, g1, s, low, copies):
    times = w.shape[1]
    width = x.shape[2]
    here = pl.BlockSpec(memory_space=pltpu.VMEM)
    there = pl.BlockSpec(memory_space=pl.ANY)
    return pl.pallas_call(
        functools.partial(rest_kernel, low),
        out_shape=(
            jax.ShapeDtypeStruct(s.shape, BF16),
            jax.ShapeDtypeStruct((copies, 8, 256), F32),
            jax.ShapeDtypeStruct((ROWS, width), BF16),
        ),
        in_specs=[here] * 5 + [there],
        out_specs=(there, here, here),
        scratch_shapes=[pltpu.VMEM((16, 256), F32), pltpu.SemaphoreType.DMA],
        input_output_aliases={5: 0},
        compiler_params=pltpu.CompilerParams(vmem_limit_bytes=16 * 2**20),
        cost_estimate=pl.CostEstimate(flops=2 * ROWS * times * width, bytes_accessed=2**22, transcendentals=0),
        name="rest",
    )(w, x, p, g0, g1, s)


def spread_to(part):
    row = lax.broadcasted_iota(jnp.int32, (HALF, ROWS), 0)
    col = lax.broadcasted_iota(jnp.int32, (HALF, ROWS), 1)
    return (col == row // NF * 2 * NF + part * NF + row % NF).astype(BF16)


def power_kernel(denominator, t_ref, *refs):
    part_refs, (o_ref, m_ref, out_ref, sem) = refs[:-4], refs[-4:]
    sums = jnp.sum(t_ref[...].astype(F32), axis=0) / denominator
    real_rows = [sums[k : k + 1, :] for k in range(PAIRS + 1)]
    imag_rows = [jnp.zeros_like(real_rows[0])] + [sums[PAIRS + k : PAIRS + k + 1, :] for k in range(1, PAIRS + 1)]
    for k in range(PAIRS + 1, NB):
        real_rows.append(turned(real_rows[NB - k], k))
        imag_rows.append(-turned(imag_rows[NB - k], k))
    block = lane_block(1)
    tables = []
    for rows in (real_rows, imag_rows):
        picked = [sum(jnp.where((block + k) % NB == b, rows[k][:, :HALF], 0.0) for k in range(NB)) for b in range(NB)]
        tables.append(jnp.concatenate(picked, axis=0).astype(BF16))
    real, imag = tables
    spread = [spread_to(part) for part in range(2)]
    from_real = dot(real, spread[0]) - dot(imag, spread[1])
    from_imag = dot(imag, spread[0]) + dot(real, spread[1])
    same = lax.broadcasted_iota(jnp.int32, (NF, ROWS), 0) == lax.broadcasted_iota(jnp.int32, (NF, ROWS), 1) % NF
    for b in range(NB):
        for part, table in enumerate((from_real, from_imag)):
            at = (2 * b + part) * NF
            row = jnp.broadcast_to(table[b : b + 1], (NF, ROWS))
            m_ref[at : at + NF, :] = jnp.where(same, row, 0.0).astype(BF16)
    stores = []
    low = 0
    for part_ref in part_refs:
        for at in range(0, part_ref.shape[1], 512):
            values = part_ref[:, at : at + 512]
            cols = pl.ds(low, values.shape[1])
            out_ref[:, low : low + values.shape[1]] = dot(m_ref[...], values)
            stores.append(pltpu.make_async_copy(out_ref.at[:, cols], o_ref.at[:, cols], sem.at[len(stores)]))
            stores[-1].start()
            low += values.shape[1]
    for store in stores:
        store.wait()


def power(t, parts, denominator):
    pts = sum(part.shape[1] for part in parts)
    here = pl.BlockSpec(memory_space=pltpu.VMEM)
    return pl.pallas_call(
        functools.partial(power_kernel, denominator),
        out_shape=jax.ShapeDtypeStruct((ROWS, pts), F32),
        in_specs=[here] * (1 + len(parts)),
        out_specs=pl.BlockSpec(memory_space=pl.ANY),
        scratch_shapes=[
            pltpu.VMEM((ROWS, ROWS), BF16),
            pltpu.VMEM((ROWS, pts), F32),
            pltpu.SemaphoreType.DMA((8,)),
        ],
        compiler_params=pltpu.CompilerParams(vmem_limit_bytes=16 * 2**20),
        name="power",
    )(t, *parts)


def to_all(t, axes):
    copies = jnp.broadcast_to(t[None], (lax.axis_size(axes), *t.shape))
    return lax.all_to_all(copies, axes, 0, 0, tiled=True)


def exchange(x, axes):
    return lax.all_to_all(x, axes, 0, 0, tiled=True)


def shards(snapshots, block_starts, kept_freqs):
    count = lax.axis_size(TA)
    local = snapshots.shape[0]
    own = snapshots.shape[2] // count
    total = own * count * lax.axis_size("zl")
    swap = [(0, 1), (1, 0)]
    x = snapshots.reshape(local, own * count)

    later = own - FIRST
    low = later - LAST
    tiles = x.reshape(local // 8, 8, 4, 2, 8, own).transpose(0, 2, 3, 4, 1, 5)
    far = 1 - lax.axis_index("zh")
    first = lax.dynamic_slice(tiles, (0, 0, far, 0, 0, later), (local // 8, 4, 1, 8, 8, FIRST))
    first = lax.ppermute(first, "zh", swap)
    pass_on = pack(x, own, 1, 0, later)
    pass_on = exchange(pass_on, PLANE)
    passed = lax.ppermute(pass_on[:, :, :low], "zh", swap)
    last = lax.ppermute(pass_on[:, :, low:], "zh", swap)
    mine = pack(x, own, 0, 0, own)
    x0 = exchange(mine, PLANE)
    side = lax.axis_index("zh")
    place = jnp.arange(local * count // 2, dtype=jnp.int32)
    times = place // 128 * 256 + place % 128
    w0 = weights(block_starts, kept_freqs, times + side * 128)
    w1 = weights(block_starts, kept_freqs, times + (1 - side) * 128)
    first, w0, w1 = lax.optimization_barrier((first, w0, w1))
    first = first.reshape(local // 8, count // 2, 8, FIRST).transpose(1, 0, 2, 3)
    first = exchange(first.reshape(count // 2, local, FIRST), PLANE)
    p0, p1 = partial(w0, x0, (low, LAST))
    s, g0, part0 = middle(w1, passed, p0, own)
    s, g1, part2 = whole(w0, w1, x0, first, s)
    s, t, part1 = rest(w1, last, p1, g0, g1, s, low, lax.axis_size(("y", "x")))
    t = exchange(t, ("y", "x")).sum(axis=0)
    t = to_all(t.astype(BF16), ("zh", "zl", "c"))
    out = power(t, (part0, part1, part2), float(NB * total))
    shape = (1, NB, 2, NF, own)
    return s.reshape(shape), out.reshape(shape)


def solution(mesh):
    split = Mesh(mesh.devices.reshape(4, 2, 4, 2, mesh.shape["ga"]), ("y", "zh", "x", "c", "zl"))
    out = P("zl", None, None, None, TA)
    return jax.shard_map(
        shards, mesh=split, in_specs=(P(TA, "zl", None), P(), P()), out_specs=(out, out), check_vma=False
    )
```

```python
import functools
import math

import jax
import jax.numpy as jnp
from jax import lax
from jax.experimental import pallas as pl
from jax.experimental.pallas import tpu as pltpu
from jax.sharding import Mesh
from jax.sharding import PartitionSpec as P


NFFT = 256
NB = 7
NF = 32
HALF = NB * NF
ROWS = 2 * HALF
PAIRS = NB // 2
TA = ("y", "zh", "x", "c")
PLANE = ("y", "x", "c")
FIRST = 768
LAST = 512
F32 = jnp.float32
BF16 = jnp.bfloat16


def weights(block_starts, kept_freqs, times):
    offset = times[None, :] - block_starts[:, None]
    inside = (offset >= 0) & (offset < NFFT)
    window = 0.5 - 0.5 * jnp.cos(2.0 * math.pi / NFFT * offset.astype(F32))
    scale = jnp.where(inside, window, 0.0)
    phase = kept_freqs[None, :, None] * jnp.where(inside, offset, 0)[:, None, :] % NFFT
    angle = 2.0 * math.pi / NFFT * phase.astype(F32)
    norm = 2.0 / math.sqrt(NFFT)
    real = scale[:, None, :] * jnp.cos(angle) * norm
    imag = -scale[:, None, :] * jnp.sin(angle) * norm
    table = jnp.stack([real, imag]).astype(BF16)
    return table.reshape(ROWS, times.shape[0])


def dot(a, b):
    return jnp.dot(a, b, preferred_element_type=F32)


def dot_t(a, b):
    return lax.dot_general(a, b, (((1,), (1,)), ((), ())), preferred_element_type=F32)


def same_freq(rows):
    row = lax.broadcasted_iota(jnp.int32, (rows, HALF), 0)
    col = lax.broadcasted_iota(jnp.int32, (rows, HALF), 1)
    return row % NF == col % NF


def pack_kernel(own, shift, low, x_ref, out_ref, buffer, in_sem, out_sem):
    side = (lax.axis_index("zh") + shift) % 2
    loads = []
    for d in range(buffer.shape[0]):
        start = ((d // 8) * 16 + d % 8) * own + low + side * (8 * own)
        cols = pl.ds(pl.multiple_of(start, 128), buffer.shape[2])
        loads.append(pltpu.make_async_copy(x_ref.at[:, cols], buffer.at[d], in_sem.at[d]))
        loads[d].start()
    stores = []
    for i in range(len(loads) // 8):
        for load in loads[8 * i : 8 * i + 8]:
            load.wait()
        rows = pl.ds(8 * i, 8)
        stores.append(pltpu.make_async_copy(buffer.at[rows], out_ref.at[rows], out_sem.at[i]))
        stores[i].start()
    for store in stores:
        store.wait()


def pack(x, own, shift, low, pts):
    count = x.shape[1] // own // 2
    shape = (count, x.shape[0], pts)
    return pl.pallas_call(
        functools.partial(pack_kernel, own, shift, low),
        out_shape=jax.ShapeDtypeStruct(shape, x.dtype),
        in_specs=[pl.BlockSpec(memory_space=pltpu.HBM)],
        out_specs=pl.BlockSpec(memory_space=pltpu.HBM),
        scratch_shapes=[
            pltpu.VMEM(shape, x.dtype),
            pltpu.SemaphoreType.DMA((count,)),
            pltpu.SemaphoreType.DMA((count // 8,)),
        ],
        compiler_params=pltpu.CompilerParams(vmem_limit_bytes=60 * 2**20),
        name="pack",
    )(x)


def emit(parts, s_ref):
    for part in range(2):
        for b in range(NB):
            start = part * HALF + b * NF
            s_ref[b * 2 * NF + part * NF : b * 2 * NF + (part + 1) * NF, :] = parts[start : start + NF]


def gram_of(parts):
    real, imag = parts[:HALF], parts[HALF:]
    return jnp.concatenate([dot_t(real, real) + dot_t(imag, imag), dot_t(imag, real)], axis=0)


def rows_of(ref):
    return ref[...].reshape(-1, ref.shape[2])


def whole_kernel(w0_ref, w1_ref, x0_ref, x1_ref, _, s_ref, out_ref, part_ref, sem):
    count = x1_ref.shape[2]
    low = x0_ref.shape[2] - count
    near = x0_ref[:, :, low:].reshape(-1, count)
    parts = (dot(w0_ref[...], near) + dot(w1_ref[...], rows_of(x1_ref))).astype(BF16)
    emit(parts, part_ref)
    save = pltpu.make_async_copy(part_ref, s_ref.at[:, pl.ds(low, count)], sem)
    save.start()
    out_ref[...] = gram_of(parts)
    save.wait()


def whole(w0, w1, x0, x1, s):
    times = w0.shape[1]
    count = x1.shape[2]
    here = pl.BlockSpec(memory_space=pltpu.VMEM)
    there = pl.BlockSpec(memory_space=pl.ANY)
    return pl.pallas_call(
        whole_kernel,
        out_shape=(
            jax.ShapeDtypeStruct(s.shape, BF16),
            jax.ShapeDtypeStruct((ROWS, HALF), F32),
            jax.ShapeDtypeStruct((ROWS, count), BF16),
        ),
        in_specs=[here] * 4 + [there],
        out_specs=(there, here, here),
        scratch_shapes=[pltpu.SemaphoreType.DMA],
        input_output_aliases={4: 0},
        compiler_params=pltpu.CompilerParams(vmem_limit_bytes=16 * 2**20),
        cost_estimate=pl.CostEstimate(flops=4 * ROWS * times * count, bytes_accessed=2**22, transcendentals=0),
        name="whole",
    )(w0, w1, x0, x1, s)


def partial_kernel(w_ref, x_ref, *p_refs):
    low = 0
    for p_ref in p_refs:
        count = p_ref.shape[1]
        p_ref[...] = dot(w_ref[...], x_ref[:, :, low : low + count].reshape(-1, count))
        low += count


def partial(w, x, counts):
    times = w.shape[1]
    here = pl.BlockSpec(memory_space=pltpu.VMEM)
    return pl.pallas_call(
        partial_kernel,
        out_shape=[jax.ShapeDtypeStruct((ROWS, count), F32) for count in counts],
        in_specs=[here, here],
        out_specs=[here] * len(counts),
        compiler_params=pltpu.CompilerParams(vmem_limit_bytes=16 * 2**20),
        cost_estimate=pl.CostEstimate(flops=2 * ROWS * times * sum(counts), bytes_accessed=2**21, transcendentals=0),
        name="partial",
    )(w, x)


def lane_block(rows):
    return lax.broadcasted_iota(jnp.int32, (rows, HALF), 1) // NF


def turned(row, k):
    lane = lax.broadcasted_iota(jnp.int32, row.shape, 1)
    near = pltpu.roll(row, 256 - k * NF, 1)
    far = pltpu.roll(row, HALF - k * NF, 1)
    return jnp.where(lane < HALF - k * NF, near, far)


def middle_kernel(w_ref, x_ref, p_ref, s_ref, out_ref, part_ref, sem):
    parts = (p_ref[...] + dot(w_ref[...], rows_of(x_ref))).astype(BF16)
    emit(parts, part_ref)
    save = pltpu.make_async_copy(part_ref, s_ref.at[:, pl.ds(0, parts.shape[1])], sem)
    save.start()
    out_ref[...] = gram_of(parts)
    save.wait()


def middle(w, x, p, pts):
    times = w.shape[1]
    width = x.shape[2]
    here = pl.BlockSpec(memory_space=pltpu.VMEM)
    return pl.pallas_call(
        middle_kernel,
        out_shape=(
            jax.ShapeDtypeStruct((ROWS, pts), BF16),
            jax.ShapeDtypeStruct((ROWS, HALF), F32),
            jax.ShapeDtypeStruct((ROWS, width), BF16),
        ),
        in_specs=[here] * 3,
        out_specs=(pl.BlockSpec(memory_space=pl.ANY), here, here),
        scratch_shapes=[pltpu.SemaphoreType.DMA],
        compiler_params=pltpu.CompilerParams(vmem_limit_bytes=16 * 2**20),
        cost_estimate=pl.CostEstimate(flops=2 * ROWS * times * width, bytes_accessed=2**22, transcendentals=0),
        name="middle",
    )(w, x, p)


def rest_kernel(low, w_ref, x_ref, p_ref, g0_ref, g1_ref, _, s_ref, t_ref, part_ref, row_ref, sem):
    width = x_ref.shape[2]
    parts = (p_ref[...] + dot(w_ref[...], rows_of(x_ref))).astype(BF16)
    emit(parts, part_ref)
    save = pltpu.make_async_copy(part_ref, s_ref.at[:, pl.ds(low, width)], sem)
    save.start()
    kept = jnp.where(same_freq(ROWS), g0_ref[...] + g1_ref[...] + gram_of(parts), 0.0)
    tables = kept.reshape(2 * NB, NF, HALF).sum(axis=1)
    block = lax.broadcasted_iota(jnp.int32, (NB, HALF), 0)
    row_ref[...] = jnp.zeros_like(row_ref)
    for k in range(NB):
        pick = (lane_block(NB) + k) % NB == block
        if k <= PAIRS:
            row_ref[k : k + 1, :HALF] = jnp.where(pick, tables[:NB], 0.0).sum(axis=0, keepdims=True)
        if k:
            row_ref[NB + k : NB + k + 1, :HALF] = jnp.where(pick, tables[NB:], 0.0).sum(axis=0, keepdims=True)
    rows = [row_ref[k : k + 1, :] for k in range(2 * NB)]
    imag = [rows[NB + k] - turned(rows[2 * NB - k], k) for k in range(1, PAIRS + 1)]
    sums = jnp.concatenate(rows[: PAIRS + 1] + imag + [jnp.zeros_like(imag[0])], axis=0)
    sums = sums.astype(BF16)
    for i in range(t_ref.shape[0]):
        t_ref[i] = sums
    save.wait()


def rest(w, x, p, g0, g1, s, low, copies):
    times = w.shape[1]
    width = x.shape[2]
    here = pl.BlockSpec(memory_space=pltpu.VMEM)
    there = pl.BlockSpec(memory_space=pl.ANY)
    return pl.pallas_call(
        functools.partial(rest_kernel, low),
        out_shape=(
            jax.ShapeDtypeStruct(s.shape, BF16),
            jax.ShapeDtypeStruct((copies, 8, 256), BF16),
            jax.ShapeDtypeStruct((ROWS, width), BF16),
        ),
        in_specs=[here] * 5 + [there],
        out_specs=(there, here, here),
        scratch_shapes=[pltpu.VMEM((16, 256), F32), pltpu.SemaphoreType.DMA],
        input_output_aliases={5: 0},
        compiler_params=pltpu.CompilerParams(vmem_limit_bytes=16 * 2**20),
        cost_estimate=pl.CostEstimate(flops=2 * ROWS * times * width, bytes_accessed=2**22, transcendentals=0),
        name="rest",
    )(w, x, p, g0, g1, s)


def spread_to(part):
    row = lax.broadcasted_iota(jnp.int32, (HALF, ROWS), 0)
    col = lax.broadcasted_iota(jnp.int32, (HALF, ROWS), 1)
    return (col == row // NF * 2 * NF + part * NF + row % NF).astype(BF16)


def power_kernel(denominator, t_ref, *refs):
    part_refs, (o_ref, m_ref, out_ref, sem) = refs[:-4], refs[-4:]
    sums = jnp.sum(t_ref[...].astype(F32), axis=0) / denominator
    real_rows = [sums[k : k + 1, :] for k in range(PAIRS + 1)]
    imag_rows = [jnp.zeros_like(real_rows[0])] + [sums[PAIRS + k : PAIRS + k + 1, :] for k in range(1, PAIRS + 1)]
    for k in range(PAIRS + 1, NB):
        real_rows.append(turned(real_rows[NB - k], k))
        imag_rows.append(-turned(imag_rows[NB - k], k))
    block = lane_block(1)
    tables = []
    for rows in (real_rows, imag_rows):
        picked = [sum(jnp.where((block + k) % NB == b, rows[k][:, :HALF], 0.0) for k in range(NB)) for b in range(NB)]
        tables += picked
    both = jnp.concatenate(tables, axis=0).astype(BF16)
    near, far = dot(both, spread_to(0)), dot(both, spread_to(1))
    from_real = near[:NB] - far[NB:]
    from_imag = near[NB:] + far[:NB]
    same = lax.broadcasted_iota(jnp.int32, (NF, ROWS), 0) == lax.broadcasted_iota(jnp.int32, (NF, ROWS), 1) % NF
    for b in range(NB):
        for part, table in enumerate((from_real, from_imag)):
            at = (2 * b + part) * NF
            row = jnp.broadcast_to(table[b : b + 1], (NF, ROWS))
            m_ref[at : at + NF, :] = jnp.where(same, row, 0.0).astype(BF16)
    stores = []
    low = 0
    for part_ref in part_refs:
        count = part_ref.shape[1]
        edges = sorted({0, count % 512, *range(count % 512, count + 1, 512)})
        for at, end in zip(edges, edges[1:]):
            values = part_ref[:, at:end]
            cols = pl.ds(low, values.shape[1])
            out_ref[:, low : low + values.shape[1]] = dot(m_ref[...], values)
            stores.append(pltpu.make_async_copy(out_ref.at[:, cols], o_ref.at[:, cols], sem.at[len(stores)]))
            stores[-1].start()
            low += values.shape[1]
    for store in stores:
        store.wait()


def power(t, parts, denominator):
    pts = sum(part.shape[1] for part in parts)
    here = pl.BlockSpec(memory_space=pltpu.VMEM)
    return pl.pallas_call(
        functools.partial(power_kernel, denominator),
        out_shape=jax.ShapeDtypeStruct((ROWS, pts), F32),
        in_specs=[here] * (1 + len(parts)),
        out_specs=pl.BlockSpec(memory_space=pl.ANY),
        scratch_shapes=[
            pltpu.VMEM((ROWS, ROWS), BF16),
            pltpu.VMEM((ROWS, pts), F32),
            pltpu.SemaphoreType.DMA((8,)),
        ],
        compiler_params=pltpu.CompilerParams(vmem_limit_bytes=16 * 2**20),
        name="power",
    )(t, *parts)


def to_all(t, axes):
    copies = jnp.broadcast_to(t[None], (lax.axis_size(axes), *t.shape))
    return lax.all_to_all(copies, axes, 0, 0, tiled=True)


def exchange(x, axes):
    return lax.all_to_all(x, axes, 0, 0, tiled=True)


def shards(snapshots, block_starts, kept_freqs):
    count = lax.axis_size(TA)
    local = snapshots.shape[0]
    own = snapshots.shape[2] // count
    total = own * count * lax.axis_size("zl")
    swap = [(0, 1), (1, 0)]
    x = snapshots.reshape(local, own * count)

    later = own - FIRST
    low = later - LAST
    first = pack(x, own, 1, later, FIRST)
    first = lax.ppermute(first, "zh", swap)
    pass_on = pack(x, own, 1, 0, later)
    pass_on = exchange(pass_on, PLANE)
    passed = lax.ppermute(pass_on[:, :, :low], "zh", swap)
    last = lax.ppermute(pass_on[:, :, low:], "zh", swap)
    mine = pack(x, own, 0, 0, own)
    x0 = exchange(mine, PLANE)
    side = lax.axis_index("zh")
    place = jnp.arange(local * count // 2, dtype=jnp.int32)
    times = place // 128 * 256 + place % 128
    w0 = weights(block_starts, kept_freqs, times + side * 128)
    w1 = weights(block_starts, kept_freqs, times + (1 - side) * 128)
    first, w0, w1 = lax.optimization_barrier((first, w0, w1))
    first = exchange(first, PLANE)
    p0, p1 = partial(w0, x0, (low, LAST))
    s, g0, part0 = middle(w1, passed, p0, own)
    s, g1, part2 = whole(w0, w1, x0, first, s)
    s, t, part1 = rest(w1, last, p1, g0, g1, s, low, lax.axis_size(("y", "x")))
    t = exchange(t, ("y", "x")).astype(F32).sum(axis=0)
    t = to_all(t.astype(BF16), ("zh", "zl", "c"))
    out = power(t, (part0, part1, part2), float(NB * total))
    shape = (1, NB, 2, NF, own)
    return s.reshape(shape), out.reshape(shape)


def solution(mesh):
    split = Mesh(mesh.devices.reshape(4, 2, 4, 2, mesh.shape["ga"]), ("y", "zh", "x", "c", "zl"))
    out = P("zl", None, None, None, TA)
    return jax.shard_map(
        shards, mesh=split, in_specs=(P(TA, "zl", None), P(), P()), out_specs=(out, out), check_vma=False
    )
```

```python
import functools
import math

import jax
import jax.numpy as jnp
from jax import lax
from jax.experimental import pallas as pl
from jax.experimental.pallas import tpu as pltpu
from jax.sharding import Mesh
from jax.sharding import PartitionSpec as P


NFFT = 256
NB = 7
NF = 32
HALF = NB * NF
ROWS = 2 * HALF
PAIRS = NB // 2
TA = ("y", "zh", "x", "c")
PLANE = ("y", "x", "c")
FIRST = 768
LAST = 512
F32 = jnp.float32
BF16 = jnp.bfloat16


def weights(block_starts, kept_freqs, times):
    offset = times[None, :] - block_starts[:, None]
    inside = (offset >= 0) & (offset < NFFT)
    window = 0.5 - 0.5 * jnp.cos(2.0 * math.pi / NFFT * offset.astype(F32))
    scale = jnp.where(inside, window, 0.0)
    phase = kept_freqs[None, :, None] * jnp.where(inside, offset, 0)[:, None, :] % NFFT
    angle = 2.0 * math.pi / NFFT * phase.astype(F32)
    norm = 2.0 / math.sqrt(NFFT)
    real = scale[:, None, :] * jnp.cos(angle) * norm
    imag = -scale[:, None, :] * jnp.sin(angle) * norm
    table = jnp.stack([real, imag]).astype(BF16)
    return table.reshape(ROWS, times.shape[0])


def dot(a, b):
    return jnp.dot(a, b, preferred_element_type=F32)


def dot_t(a, b):
    return lax.dot_general(a, b, (((1,), (1,)), ((), ())), preferred_element_type=F32)


def same_freq(rows):
    row = lax.broadcasted_iota(jnp.int32, (rows, HALF), 0)
    col = lax.broadcasted_iota(jnp.int32, (rows, HALF), 1)
    return row % NF == col % NF


def pack_kernel(shift, low, x_ref, out_ref, buffer, in_sem, out_sem):
    side = (lax.axis_index("zh") + shift) % 2
    runs, _, halves, _, pts = buffer.shape
    loads = []
    for y in range(runs):
        for half in range(halves):
            source = x_ref.at[half, y, side, :, :, pl.ds(low, pts)]
            loads.append(pltpu.make_async_copy(source, buffer.at[y, :, half], in_sem.at[y * halves + half]))
            loads[-1].start()
    stores = []
    for y in range(runs):
        for load in loads[y * halves : (y + 1) * halves]:
            load.wait()
        stores.append(pltpu.make_async_copy(buffer.at[y], out_ref.at[y], out_sem.at[y]))
        stores[y].start()
    for store in stores:
        store.wait()


def pack(x, own, shift, low, pts):
    local = x.shape[0]
    tiles = x.reshape(local // 8, 8, 4, 2, 8, own).transpose(0, 2, 3, 4, 1, 5)
    shape = (4, 8, local // 8, 8, pts)
    packed = pl.pallas_call(
        functools.partial(pack_kernel, shift, low),
        out_shape=jax.ShapeDtypeStruct(shape, x.dtype),
        in_specs=[pl.BlockSpec(memory_space=pltpu.HBM)],
        out_specs=pl.BlockSpec(memory_space=pltpu.HBM),
        scratch_shapes=[
            pltpu.VMEM(shape, x.dtype),
            pltpu.SemaphoreType.DMA((4 * (local // 8),)),
            pltpu.SemaphoreType.DMA((4,)),
        ],
        compiler_params=pltpu.CompilerParams(vmem_limit_bytes=60 * 2**20),
        name="pack",
    )(tiles)
    return packed.reshape(32, local, pts)


def emit(parts, s_ref):
    for part in range(2):
        for b in range(NB):
            start = part * HALF + b * NF
            s_ref[b * 2 * NF + part * NF : b * 2 * NF + (part + 1) * NF, :] = parts[start : start + NF]


def gram_of(parts):
    real, imag = parts[:HALF], parts[HALF:]
    return jnp.concatenate([dot_t(real, real) + dot_t(imag, imag), dot_t(imag, real)], axis=0)


def rows_of(ref):
    return ref[...].reshape(-1, ref.shape[2])


def whole_kernel(w0_ref, w1_ref, x0_ref, x1_ref, _, s_ref, out_ref, part_ref, sem):
    count = x1_ref.shape[2]
    low = x0_ref.shape[2] - count
    near = x0_ref[:, :, low:].reshape(-1, count)
    parts = (dot(w0_ref[...], near) + dot(w1_ref[...], rows_of(x1_ref))).astype(BF16)
    emit(parts, part_ref)
    save = pltpu.make_async_copy(part_ref, s_ref.at[:, pl.ds(low, count)], sem)
    save.start()
    out_ref[...] = gram_of(parts)
    save.wait()


def whole(w0, w1, x0, x1, s):
    times = w0.shape[1]
    count = x1.shape[2]
    here = pl.BlockSpec(memory_space=pltpu.VMEM)
    there = pl.BlockSpec(memory_space=pl.ANY)
    return pl.pallas_call(
        whole_kernel,
        out_shape=(
            jax.ShapeDtypeStruct(s.shape, BF16),
            jax.ShapeDtypeStruct((ROWS, HALF), F32),
            jax.ShapeDtypeStruct((ROWS, count), BF16),
        ),
        in_specs=[here] * 4 + [there],
        out_specs=(there, here, here),
        scratch_shapes=[pltpu.SemaphoreType.DMA],
        input_output_aliases={4: 0},
        compiler_params=pltpu.CompilerParams(vmem_limit_bytes=16 * 2**20),
        cost_estimate=pl.CostEstimate(flops=4 * ROWS * times * count, bytes_accessed=2**22, transcendentals=0),
        name="whole",
    )(w0, w1, x0, x1, s)


def partial_kernel(w_ref, x_ref, *p_refs):
    low = 0
    for p_ref in p_refs:
        count = p_ref.shape[1]
        p_ref[...] = dot(w_ref[...], x_ref[:, :, low : low + count].reshape(-1, count))
        low += count


def partial(w, x, counts):
    times = w.shape[1]
    here = pl.BlockSpec(memory_space=pltpu.VMEM)
    return pl.pallas_call(
        partial_kernel,
        out_shape=[jax.ShapeDtypeStruct((ROWS, count), F32) for count in counts],
        in_specs=[here, here],
        out_specs=[here] * len(counts),
        compiler_params=pltpu.CompilerParams(vmem_limit_bytes=16 * 2**20),
        cost_estimate=pl.CostEstimate(flops=2 * ROWS * times * sum(counts), bytes_accessed=2**21, transcendentals=0),
        name="partial",
    )(w, x)


def lane_block(rows):
    return lax.broadcasted_iota(jnp.int32, (rows, HALF), 1) // NF


def turned(row, k):
    lane = lax.broadcasted_iota(jnp.int32, row.shape, 1)
    near = pltpu.roll(row, 256 - k * NF, 1)
    far = pltpu.roll(row, HALF - k * NF, 1)
    return jnp.where(lane < HALF - k * NF, near, far)


def middle_kernel(w_ref, x_ref, p_ref, s_ref, out_ref, part_ref, sem):
    parts = (p_ref[...] + dot(w_ref[...], rows_of(x_ref))).astype(BF16)
    emit(parts, part_ref)
    save = pltpu.make_async_copy(part_ref, s_ref.at[:, pl.ds(0, parts.shape[1])], sem)
    save.start()
    out_ref[...] = gram_of(parts)
    save.wait()


def middle(w, x, p, pts):
    times = w.shape[1]
    width = x.shape[2]
    here = pl.BlockSpec(memory_space=pltpu.VMEM)
    return pl.pallas_call(
        middle_kernel,
        out_shape=(
            jax.ShapeDtypeStruct((ROWS, pts), BF16),
            jax.ShapeDtypeStruct((ROWS, HALF), F32),
            jax.ShapeDtypeStruct((ROWS, width), BF16),
        ),
        in_specs=[here] * 3,
        out_specs=(pl.BlockSpec(memory_space=pl.ANY), here, here),
        scratch_shapes=[pltpu.SemaphoreType.DMA],
        compiler_params=pltpu.CompilerParams(vmem_limit_bytes=16 * 2**20),
        cost_estimate=pl.CostEstimate(flops=2 * ROWS * times * width, bytes_accessed=2**22, transcendentals=0),
        name="middle",
    )(w, x, p)


def rest_kernel(low, w_ref, x_ref, p_ref, g0_ref, g1_ref, _, s_ref, t_ref, part_ref, row_ref, sem):
    width = x_ref.shape[2]
    parts = (p_ref[...] + dot(w_ref[...], rows_of(x_ref))).astype(BF16)
    emit(parts, part_ref)
    save = pltpu.make_async_copy(part_ref, s_ref.at[:, pl.ds(low, width)], sem)
    save.start()
    kept = jnp.where(same_freq(ROWS), g0_ref[...] + g1_ref[...] + gram_of(parts), 0.0)
    tables = kept.reshape(2 * NB, NF, HALF).sum(axis=1)
    block = lax.broadcasted_iota(jnp.int32, (NB, HALF), 0)
    row_ref[...] = jnp.zeros_like(row_ref)
    for k in range(NB):
        pick = (lane_block(NB) + k) % NB == block
        if k <= PAIRS:
            row_ref[k : k + 1, :HALF] = jnp.where(pick, tables[:NB], 0.0).sum(axis=0, keepdims=True)
        if k:
            row_ref[NB + k : NB + k + 1, :HALF] = jnp.where(pick, tables[NB:], 0.0).sum(axis=0, keepdims=True)
    rows = [row_ref[k : k + 1, :] for k in range(2 * NB)]
    imag = [rows[NB + k] - turned(rows[2 * NB - k], k) for k in range(1, PAIRS + 1)]
    sums = jnp.concatenate(rows[: PAIRS + 1] + imag + [jnp.zeros_like(imag[0])], axis=0)
    sums = sums.astype(BF16)
    for i in range(t_ref.shape[0]):
        t_ref[i] = sums
    save.wait()


def rest(w, x, p, g0, g1, s, low, copies):
    times = w.shape[1]
    width = x.shape[2]
    here = pl.BlockSpec(memory_space=pltpu.VMEM)
    there = pl.BlockSpec(memory_space=pl.ANY)
    return pl.pallas_call(
        functools.partial(rest_kernel, low),
        out_shape=(
            jax.ShapeDtypeStruct(s.shape, BF16),
            jax.ShapeDtypeStruct((copies, 8, 256), BF16),
            jax.ShapeDtypeStruct((ROWS, width), BF16),
        ),
        in_specs=[here] * 5 + [there],
        out_specs=(there, here, here),
        scratch_shapes=[pltpu.VMEM((16, 256), F32), pltpu.SemaphoreType.DMA],
        input_output_aliases={5: 0},
        compiler_params=pltpu.CompilerParams(vmem_limit_bytes=16 * 2**20),
        cost_estimate=pl.CostEstimate(flops=2 * ROWS * times * width, bytes_accessed=2**22, transcendentals=0),
        name="rest",
    )(w, x, p, g0, g1, s)


def spread_to(part):
    row = lax.broadcasted_iota(jnp.int32, (HALF, ROWS), 0)
    col = lax.broadcasted_iota(jnp.int32, (HALF, ROWS), 1)
    return (col == row // NF * 2 * NF + part * NF + row % NF).astype(BF16)


def power_kernel(denominator, t_ref, *refs):
    part_refs, (o_ref, m_ref, out_ref, sem) = refs[:-4], refs[-4:]
    sums = jnp.sum(t_ref[...].astype(F32), axis=0) / denominator
    real_rows = [sums[k : k + 1, :] for k in range(PAIRS + 1)]
    imag_rows = [jnp.zeros_like(real_rows[0])] + [sums[PAIRS + k : PAIRS + k + 1, :] for k in range(1, PAIRS + 1)]
    for k in range(PAIRS + 1, NB):
        real_rows.append(turned(real_rows[NB - k], k))
        imag_rows.append(-turned(imag_rows[NB - k], k))
    block = lane_block(1)
    tables = []
    for rows in (real_rows, imag_rows):
        picked = [sum(jnp.where((block + k) % NB == b, rows[k][:, :HALF], 0.0) for k in range(NB)) for b in range(NB)]
        tables += picked
    both = jnp.concatenate(tables, axis=0).astype(BF16)
    near, far = dot(both, spread_to(0)), dot(both, spread_to(1))
    from_real = near[:NB] - far[NB:]
    from_imag = near[NB:] + far[:NB]
    same = lax.broadcasted_iota(jnp.int32, (NF, ROWS), 0) == lax.broadcasted_iota(jnp.int32, (NF, ROWS), 1) % NF
    for b in range(NB):
        for part, table in enumerate((from_real, from_imag)):
            at = (2 * b + part) * NF
            row = jnp.broadcast_to(table[b : b + 1], (NF, ROWS))
            m_ref[at : at + NF, :] = jnp.where(same, row, 0.0).astype(BF16)
    stores = []
    low = 0
    for part_ref in part_refs:
        count = part_ref.shape[1]
        edges = sorted({0, count % 512, *range(count % 512, count + 1, 512)})
        for at, end in zip(edges, edges[1:]):
            values = part_ref[:, at:end]
            cols = pl.ds(low, values.shape[1])
            out_ref[:, low : low + values.shape[1]] = dot(m_ref[...], values)
            stores.append(pltpu.make_async_copy(out_ref.at[:, cols], o_ref.at[:, cols], sem.at[len(stores)]))
            stores[-1].start()
            low += values.shape[1]
    for store in stores:
        store.wait()


def power(t, parts, denominator):
    pts = sum(part.shape[1] for part in parts)
    here = pl.BlockSpec(memory_space=pltpu.VMEM)
    return pl.pallas_call(
        functools.partial(power_kernel, denominator),
        out_shape=jax.ShapeDtypeStruct((ROWS, pts), F32),
        in_specs=[here] * (1 + len(parts)),
        out_specs=pl.BlockSpec(memory_space=pl.ANY),
        scratch_shapes=[
            pltpu.VMEM((ROWS, ROWS), BF16),
            pltpu.VMEM((ROWS, pts), F32),
            pltpu.SemaphoreType.DMA((8,)),
        ],
        compiler_params=pltpu.CompilerParams(vmem_limit_bytes=16 * 2**20),
        name="power",
    )(t, *parts)


def to_all(t, axes):
    copies = jnp.broadcast_to(t[None], (lax.axis_size(axes), *t.shape))
    return lax.all_to_all(copies, axes, 0, 0, tiled=True)


def exchange(x, axes):
    return lax.all_to_all(x, axes, 0, 0, tiled=True)


def shards(snapshots, block_starts, kept_freqs):
    count = lax.axis_size(TA)
    local = snapshots.shape[0]
    own = snapshots.shape[2] // count
    total = own * count * lax.axis_size("zl")
    swap = [(0, 1), (1, 0)]
    x = snapshots.reshape(local, own * count)

    later = own - FIRST
    low = later - LAST
    first = pack(x, own, 1, later, FIRST)
    first = lax.ppermute(first, "zh", swap)
    pass_on = pack(x, own, 1, 0, later)
    pass_on = exchange(pass_on, PLANE)
    passed = lax.ppermute(pass_on[:, :, :low], "zh", swap)
    last = lax.ppermute(pass_on[:, :, low:], "zh", swap)
    mine = pack(x, own, 0, 0, own)
    x0 = exchange(mine, PLANE)
    side = lax.axis_index("zh")
    place = jnp.arange(local * count // 2, dtype=jnp.int32)
    times = place // 128 * 256 + place % 128
    w0 = weights(block_starts, kept_freqs, times + side * 128)
    w1 = weights(block_starts, kept_freqs, times + (1 - side) * 128)
    first, w0, w1 = lax.optimization_barrier((first, w0, w1))
    first = exchange(first, PLANE)
    p0, p1 = partial(w0, x0, (low, LAST))
    s, g0, part0 = middle(w1, passed, p0, own)
    s, g1, part2 = whole(w0, w1, x0, first, s)
    s, t, part1 = rest(w1, last, p1, g0, g1, s, low, lax.axis_size(("y", "x")))
    t = exchange(t, ("y", "x")).astype(F32).sum(axis=0)
    t = to_all(t.astype(BF16), ("zh", "zl", "c"))
    out = power(t, (part0, part1, part2), float(NB * total))
    shape = (1, NB, 2, NF, own)
    return s.reshape(shape), out.reshape(shape)


def solution(mesh):
    split = Mesh(mesh.devices.reshape(4, 2, 4, 2, mesh.shape["ga"]), ("y", "zh", "x", "c", "zl"))
    out = P("zl", None, None, None, TA)
    return jax.shard_map(
        shards, mesh=split, in_specs=(P(TA, "zl", None), P(), P()), out_specs=(out, out), check_vma=False
    )
```
